32 devices in a mesh: stage: 4 (over z), data: 8 (over y, x, core).
Axes of the slice: x: 2, y: 2, z: 4, core: 2. Of those that a mesh axis runs over, the one named last changes fastest.
Arguments:
- inputs: bfloat16 [32, 64, 768], P('data')
- targets: bfloat16 [32, 64, 768], P('data')
- w_up: bfloat16 [24, 768, 3072], P('stage')
- w_down: bfloat16 [24, 3072, 768], P('stage')
Outputs:
- output 1: float32 [], replicated
- output 2: float32 [24, 768, 3072], P('stage', 'data')
- output 3: float32 [24, 3072, 768], P('stage', None, 'data')
All inputs are finite; a program needn't handle non-finite values.
Results may differ from the reference program's by a relative error of at most 0.00946734.
Values are sent between devices in bfloat16 or wider.
A program may use at most 1 GiB of HBM per device.

```python
import jax
import jax.numpy as jnp
from jax import lax

DATA_REPLICAS = 8
MICRO = 4
TOKENS = 64
D_MODEL = 768
FFN = 3072
LAYERS = 24


def setup_inputs(seed: int = 0) -> dict:
    root_key = jax.random.key(seed)
    key_inputs, key_targets, key_up, key_down = jax.random.split(root_key, 4)
    n_rows = DATA_REPLICAS * MICRO
    inputs = jax.random.normal(key_inputs, (n_rows, TOKENS, D_MODEL), jnp.float32)
    targets = jax.random.normal(key_targets, (n_rows, TOKENS, D_MODEL), jnp.float32)
    w_up = jax.random.normal(key_up, (LAYERS, D_MODEL, FFN), jnp.float32) * D_MODEL ** -0.5
    w_down = jax.random.normal(key_down, (LAYERS, FFN, D_MODEL), jnp.float32) * 1.5 * (FFN * LAYERS) ** -0.5
    return {'inputs': inputs.astype(jnp.bfloat16), 'targets': targets.astype(jnp.bfloat16), 'w_up': w_up.astype(jnp.bfloat16), 'w_down': w_down.astype(jnp.bfloat16)}


def layer_forward(h_in, w_up, w_down):
    pre_act = jnp.dot(h_in, w_up, preferred_element_type=jnp.float32)
    gelu_out = jax.nn.gelu(pre_act).astype(jnp.bfloat16)
    branch = jnp.dot(gelu_out, w_down, preferred_element_type=jnp.float32)
    return (h_in.astype(jnp.float32) + branch).astype(jnp.bfloat16)


def layer_backward(h_in, grad_out, w_up, w_down):
    pre_act = jnp.dot(h_in, w_up, preferred_element_type=jnp.float32)
    gelu_full, gelu_vjp = jax.vjp(jax.nn.gelu, pre_act)
    gelu_out = gelu_full.astype(jnp.bfloat16)
    g_down = jnp.dot(gelu_out.T, grad_out, preferred_element_type=jnp.float32)
    grad_act = jnp.dot(grad_out, w_down.T, preferred_element_type=jnp.float32).astype(jnp.bfloat16)
    grad_pre = gelu_vjp(grad_act.astype(jnp.float32))[0].astype(jnp.bfloat16)
    g_up = jnp.dot(h_in.T, grad_pre, preferred_element_type=jnp.float32)
    back_prod = jnp.dot(grad_pre, w_up.T, preferred_element_type=jnp.float32)
    grad_in = (grad_out.astype(jnp.float32) + back_prod).astype(jnp.bfloat16)
    return grad_in, g_up, g_down


def reference(inputs, targets, w_up, w_down):
    inv_total = 1.0 / (inputs.shape[0] * inputs.shape[1])

    def fwd_step(h_cur, weights):
        return layer_forward(h_cur, weights[0], weights[1]), h_cur

    def bwd_step(grad_cur, packed):
        grad_in, g_up, g_down = layer_backward(packed[0], grad_cur, packed[1], packed[2])
        return grad_in, (g_up, g_down)

    def one_micro(loop_state, mb_pair):
        acc_up, acc_down, loss_sum = loop_state
        h_last, layer_ins = lax.scan(fwd_step, mb_pair[0], (w_up, w_down))
        resid_diff = h_last.astype(jnp.float32) - mb_pair[1].astype(jnp.float32)
        top_grad = (resid_diff * inv_total).astype(jnp.bfloat16)
        scan_out = lax.scan(bwd_step, top_grad, (layer_ins, w_up, w_down), reverse=True)
        grads_up, grads_down = scan_out[1]
        new_state = (acc_up + grads_up, acc_down + grads_down, loss_sum + jnp.sum(resid_diff * resid_diff))
        return new_state, None

    init_state = (jnp.zeros(w_up.shape, jnp.float32), jnp.zeros(w_down.shape, jnp.float32), jnp.zeros((), jnp.float32))
    final_state = lax.scan(one_micro, init_state, (inputs, targets))[0]
    return final_state[2] * (0.5 * inv_total), final_state[0], final_state[1]
```

```python
import functools

import jax
import jax.numpy as jnp
from jax import lax
from jax.experimental import pallas as pl
from jax.experimental.pallas import tpu as pltpu
from jax.sharding import PartitionSpec as P

bf16, f32 = jnp.bfloat16, jnp.float32
MESH = pl.DeviceIdType.MESH
NT = (((1,), (1,)), ((), ()))
C0 = 0.7978845608028654
C1 = C0 * 0.044715
D, F = 768, 3072
CH, PR = 128, 256
NL = 3
DS = 192
FB = 768
NSTEP = 18


def dot(a, b):
    return jnp.dot(a, b, preferred_element_type=f32)


def dot_nt(a, b):
    return lax.dot_general(a, b, NT, preferred_element_type=f32)


def gelu(u):
    t = jnp.tanh(u * (C0 + C1 * (u * u)))
    hu = 0.5 * u
    return hu + hu * t


def gelu_and_slope(u):
    s = u * u
    t = jnp.tanh(u * (C0 + C1 * s))
    a = 1.0 + t
    g = (0.5 * u) * a
    return g, 0.5 * a + g * ((1.0 - t) * (C0 + (3.0 * C1) * s))


def kernel(inv_total, x_in, y_in, w_up, w_down,
           loss_out, out_up, out_down, u_hbm,
           w1, w2, hs, es, acc1, acc2, ub, gs, qs, hT, hcur, ecur, eout, tgt, sel, ltile, lbuf, lmine,
           wsem, hrecv, erecv, trecv, lrecv, xsend, hfwd, efwd, hsend, esend, tsend, lsend, lchain_s, lchain_r,
           osem, isem, xo_s, xo_r, lo_s):
    s = lax.axis_index("stage")
    d = lax.axis_index("data")
    c = d % 2
    q = d // 2
    k = 2 * s + c
    nxt = (s + c, d + 1 - 2 * c)
    prv = (s - 1 + c, d + 1 - 2 * c)
    partner = (s, d + 1 - 2 * c)
    peers = [(s, ((q + p) % 4) * 2 + c) for p in (1, 2, 3)]

    def rcopy(src, dst, ss, rs, dev):
        return pltpu.make_async_remote_copy(src_ref=src, dst_ref=dst, send_sem=ss, recv_sem=rs, device_id=dev, device_id_type=MESH)

    def lcopy(src, dst, sem):
        return pltpu.make_async_copy(src, dst, sem)

    bar = pltpu.get_barrier_semaphore()
    for dev in peers:
        pl.semaphore_signal(bar, inc=1, device_id=dev, device_id_type=MESH)

    @pl.when(k < 7)
    def _():
        pl.semaphore_signal(bar, inc=1, device_id=nxt, device_id_type=MESH)

    @pl.when(k > 0)
    def _():
        pl.semaphore_signal(bar, inc=1, device_id=prv, device_id_type=MESH)

    def wcopy(l, m):
        if m == 0:
            return lcopy(w_up.at[NL * c + l], w1.at[l], wsem.at[l, 0])
        return lcopy(w_down.at[NL * c + l], w2.at[l], wsem.at[l, 1])

    for l in range(NL):
        for m in range(2):
            wcopy(l, m).start()

    def slot(ref, ch):
        return ref.at[ch // 2, pl.ds(pl.multiple_of((ch % 2) * CH, CH), CH), :]

    own0 = 4 * q

    @pl.when(k == 0)
    def _():
        for j in range(2):
            lcopy(x_in.at[pl.ds(j * CH, CH), :], slot(hs, own0 + j), hrecv.at[own0 + j]).start()

    @pl.when(k == 7)
    def _():
        lcopy(y_in, tgt.at[1], trecv.at[1]).start()

    row = lax.broadcasted_iota(jnp.int32, (DS, D), 0)
    col = lax.broadcasted_iota(jnp.int32, (DS, D), 1)
    sel[...] = jnp.where(col == row + DS * q, 1.0, 0.0).astype(bf16)
    ltile[...] = jnp.zeros_like(ltile)

    def zero(i, carry):
        r = pl.ds(pl.multiple_of(i * 8, 8), 8)
        for l in range(NL):
            acc1[l, r, :] = jnp.zeros((8, F), f32)
            acc2[l, r, :] = jnp.zeros((8, F), f32)
        return carry

    lax.fori_loop(0, DS // 8, zero, 0)

    pl.semaphore_wait(bar, 3 + jnp.where(k < 7, 1, 0) + jnp.where(k > 0, 1, 0))

    def xcopy(j):
        return rcopy(x_in.at[pl.ds(j * CH, CH), :], slot(hs, own0 + 2 + j), xsend.at[j], hrecv.at[own0 + 2 + j], partner)

    def tcopy():
        return rcopy(y_in, tgt.at[0], tsend.at[0], trecv.at[0], partner)

    @pl.when(k == 1)
    def _():
        xcopy(0).start()
        xcopy(1).start()

    @pl.when(k == 6)
    def _():
        tcopy().start()

    def h_fwd(j, p):
        ch = own0 + j
        return rcopy(slot(hs, ch), slot(hs, ch), hfwd.at[j, p], hrecv.at[ch], peers[p])

    def e_fwd(jp, p):
        pr = 2 * q + jp
        return rcopy(es.at[pr], es.at[pr], efwd.at[jp, p], erecv.at[pr], peers[p])

    def h_out(j):
        return rcopy(slot(tgt, j), slot(hs, own0 + j), hsend.at[j], hrecv.at[own0 + j], nxt)

    def e_out(jp):
        return rcopy(eout.at[jp], es.at[2 * q + jp], esend.at[jp], erecv.at[2 * q + jp], prv)

    def l_peer(p):
        return rcopy(lmine, lbuf.at[q], lsend.at[p], lrecv.at[q], peers[p])

    def l_chain():
        return rcopy(loss_out, loss_out, lchain_s, lchain_r, prv)

    def wait_h(ch):
        rcopy(slot(hs, ch), slot(hs, ch), hfwd.at[0, 0], hrecv.at[ch], peers[0]).wait_recv()

    def wait_e(pr):
        rcopy(es.at[pr], es.at[pr], efwd.at[0, 0], erecv.at[pr], peers[0]).wait_recv()

    def u_out_own(l, ch, b):
        return lcopy(ub.at[b, pl.ds(0, CH), :], u_hbm.at[l, ch // 2, pl.ds(pl.multiple_of((ch % 2) * CH, CH), CH), :], osem.at[b])

    def u_out(l, pr, b):
        return lcopy(ub.at[b], u_hbm.at[l, pr], osem.at[b])

    def u_in(l, pr, b):
        return lcopy(u_hbm.at[l, pr], ub.at[b], isem.at[b])

    early = jnp.where(k == 6, 1, jnp.minimum(6, 2 * (7 - k)))
    last = k == 7

    def is_f_own(t):
        return jnp.where(last, (t < 2) | (t == 3) | (t == 4), t < 4)

    def f_own_j(t):
        return jnp.where(last & (t > 2), t - 1, t)

    def is_b_own(t):
        return jnp.where(last, (t == 2) | (t == 5), (t >= 4 + early) & (t < 6 + early))

    def b_own_j(t):
        return jnp.where(last, t // 4, t - 4 - early)

    def is_b_oth(t):
        return (t >= 12) & (t < NSTEP)

    def is_b(t):
        return is_b_own(t) | is_b_oth(t)

    def is_f_oth(t):
        return jnp.logical_not(is_f_own(t) | is_b(t)) & (t >= 2)

    def f_oth_i(t):
        return jnp.where(last, t - 6, jnp.where(t < 4 + early, t - 4, t - 6))

    def oth_pair(i):
        return 2 * ((q + 1 + i % 3) % 4) + i // 3

    def b_pair(t):
        return jnp.where(is_b_own(t), 2 * q + b_own_j(t), oth_pair(t - 12))

    def up_half(l, M, pr, off, b):
        h = hcur[0:M, :]
        hT[l, pr, :, pl.ds(off, M)] = dot_nt(sel[...], h).astype(bf16)
        for i in range(F // FB):
            o = i * FB
            u = dot(h, w1[l, :, o:o + FB])
            ub[b, 0:M, o:o + FB] = u
            gs[0:M, o:o + FB] = gelu(u).astype(bf16)

    def down_half(l, M):
        v = dot(gs[0:M, :], w2[l])
        hcur[0:M, :] = (hcur[0:M, :].astype(f32) + v).astype(bf16)

    def f_own(t):
        j = f_own_j(t)
        ch = own0 + j
        wait_h(ch)
        for p in range(3):
            h_fwd(j, p).start()
        off = pl.multiple_of((j % 2) * CH, CH)
        hcur[0:CH, :] = hs[ch // 2, pl.ds(off, CH), :]

        def layer(l, carry):
            b = l % 2

            @pl.when(t == 0)
            def _():
                lcopy(w_up.at[NL * c + l], w1.at[l], wsem.at[l, 0]).wait()
                lcopy(w_down.at[NL * c + l], w2.at[l], wsem.at[l, 1]).wait()

            @pl.when(l == 2)
            def _():
                u_out_own(0, ch, 0).wait()

            up_half(l, CH, ch // 2, off, b)
            u_out_own(l, ch, b).start()
            down_half(l, CH)
            return carry

        lax.fori_loop(0, NL, layer, 0)

        @pl.when(k < 7)
        def _():
            tgt[j // 2, pl.ds(off, CH), :] = hcur[0:CH, :]
            h_out(j).start()

        @pl.when(k == 7)
        def _():
            @pl.when(j == 0)
            def _():
                rcopy(y_in, tgt.at[0], tsend.at[0], trecv.at[0], partner).wait_recv()

            @pl.when(j == 2)
            def _():
                lcopy(y_in, tgt.at[1], trecv.at[1]).wait()

            diff = hcur[0:CH, :].astype(f32) - tgt[j // 2, pl.ds(off, CH), :].astype(f32)
            es[ch // 2, pl.ds(off, CH), :] = (diff * inv_total).astype(bf16)
            sq = jnp.sum((diff * diff).reshape(CH // 8, 8, D), axis=0)
            ltile[...] += sum(sq[:, i * 128:(i + 1) * 128] for i in range(D // 128))

            @pl.when(j == 3)
            def _():
                lmine[...] = ltile[...]

        u_out_own(1, ch, 1).wait()
        u_out_own(2, ch, 0).wait()

    def f_oth(t):
        pr = oth_pair(f_oth_i(t))
        wait_h(2 * pr)
        wait_h(2 * pr + 1)
        hcur[...] = hs[pr]

        def layer(l, carry):
            b = (t + l) % 2

            @pl.when((l == 1) & is_f_oth(t - 1))
            def _():
                u_out(2, 0, b).wait()

            @pl.when(l == 2)
            def _():
                u_out(0, pr, b).wait()

            up_half(l, PR, pr, 0, b)
            u_out(l, pr, b).start()

            @pl.when(l < 2)
            def _():
                down_half(l, PR)

            return carry

        lax.fori_loop(0, NL, layer, 0)
        u_out(1, pr, (t + 1) % 2).wait()

    def b_step(t):
        own = is_b_own(t)
        jp = b_own_j(t)
        pr = b_pair(t)

        @pl.when(is_f_oth(t - 1))
        def _():
            u_out(2, 0, (t + 1) % 2).wait()

        @pl.when(jnp.logical_not(is_b(t - 1)))
        def _():
            u_in(2, pr, t % 2).start()

        @pl.when(jnp.logical_not(own & last))
        def _():
            wait_e(pr)

        ecur[...] = es[pr]

        def layer(li, carry):
            l = 2 - li
            b = (t + li) % 2
            u_in(l, pr, b).wait()

            @pl.when(li < 2)
            def _():
                u_in(l - 1, pr, 1 - b).start()

            @pl.when((li == 2) & is_b(t + 1))
            def _():
                u_in(2, b_pair(t + 1), 1 - b).start()

            e = ecur[...]
            eT = dot_nt(sel[...], e).astype(bf16)
            hTl = hT[l, pr]
            for i in range(F // FB):
                o = i * FB
                p = dot_nt(e, w2[l, o:o + FB, :]).astype(bf16).astype(f32)
                g, slope = gelu_and_slope(ub[b, :, o:o + FB])
                qq = (p * slope).astype(bf16)
                qs[:, o:o + FB] = qq
                acc1[l, :, o:o + FB] += dot(hTl, qq)
                acc2[l, :, o:o + FB] += dot(eT, g.astype(bf16))

            @pl.when(own | (l > 0))
            def _():
                dh = dot_nt(qs[...], w1[l])
                ecur[...] = (ecur[...].astype(f32) + dh).astype(bf16)

            @pl.when(own & (li == 0))
            def _():
                for p_ in range(3):
                    e_fwd(jp, p_).start()

            @pl.when(t == NSTEP - 1)
            def _():
                for cp in final_copies(l):
                    cp.start()

            return carry

        lax.fori_loop(0, NL, layer, 0)

        @pl.when(own)
        def _():
            @pl.when(k > 0)
            def _():
                eout[jp] = ecur[...]
                e_out(jp).start()

            @pl.when(jp == 1)
            def _():
                @pl.when(k == 7)
                def _():
                    for p_ in range(3):
                        l_peer(p_).start()
                    for p_ in range(3):
                        qq_ = (q + 1 + p_) % 4
                        rcopy(lmine, lbuf.at[qq_], lsend.at[p_], lrecv.at[qq_], peers[p_]).wait_recv()
                    lbuf[q] = lmine[...]
                    tot = (lbuf[0] + lbuf[1]) + (lbuf[2] + lbuf[3])
                    loss_out[...] = jnp.zeros((8, 128), f32) + jnp.sum(tot) * (0.5 * inv_total)

                @pl.when(k < 7)
                def _():
                    l_chain().wait_recv()

                @pl.when(k > 0)
                def _():
                    l_chain().start()

    half_own = pl.ds(pl.multiple_of(96 * c, 8), 96)
    half_oth = pl.ds(pl.multiple_of(96 * (1 - c), 8), 96)

    def final_copies(l):
        L = NL * c + l
        return [
            rcopy(acc1.at[l, half_oth, :], out_up.at[L], xo_s.at[l, 0], xo_r.at[l, 0], partner),
            rcopy(acc2.at[l, half_oth, :], out_down.at[L], xo_s.at[l, 1], xo_r.at[l, 1], partner),
            lcopy(acc1.at[l, half_own, :], out_up.at[L], lo_s.at[l, 0]),
            lcopy(acc2.at[l, half_own, :], out_down.at[L], lo_s.at[l, 1]),
        ]

    def step(t, carry):
        @pl.when(is_f_own(t))
        def _():
            f_own(t)

        @pl.when(is_f_oth(t))
        def _():
            f_oth(t)

        @pl.when(is_b(t))
        def _():
            b_step(t)

        return carry

    lax.fori_loop(0, NSTEP, step, 0)

    for j in range(4):
        for p in range(3):
            h_fwd(j, p).wait_send()
    for jp in range(2):
        for p in range(3):
            e_fwd(jp, p).wait_send()

    @pl.when(k < 7)
    def _():
        for j in range(4):
            h_out(j).wait_send()

    @pl.when(k > 0)
    def _():
        for jp in range(2):
            e_out(jp).wait_send()
        l_chain().wait_send()

    @pl.when(k == 1)
    def _():
        xcopy(0).wait_send()
        xcopy(1).wait_send()

    @pl.when(k == 6)
    def _():
        tcopy().wait_send()

    @pl.when(k == 7)
    def _():
        for p in range(3):
            l_peer(p).wait_send()

    for l in range(NL):
        L = NL * (1 - c) + l
        rcopy(acc1.at[l, half_oth, :], out_up.at[L], xo_s.at[l, 0], xo_r.at[l, 0], partner).wait_recv()
        rcopy(acc2.at[l, half_oth, :], out_down.at[L], xo_s.at[l, 1], xo_r.at[l, 1], partner).wait_recv()
        r1, r2, l1, l2 = final_copies(l)
        r1.wait_send()
        r2.wait_send()
        l1.wait()
        l2.wait()


def solution(mesh):
    n_data = mesh.shape["data"]

    def per_device(inputs, targets, w_up, w_down):
        n_micro, n_tok, width = inputs.shape
        inv_total = 1.0 / (n_data * n_micro * n_tok)
        x = inputs.reshape(n_micro * n_tok, width)
        y = targets.reshape(n_micro * n_tok, width)
        V = pltpu.VMEM
        DMA = pltpu.SemaphoreType.DMA
        anyspec = pl.BlockSpec(memory_space=pl.ANY)
        loss, g_up, g_down, _ = pl.pallas_call(
            functools.partial(kernel, inv_total),
            out_shape=(
                jax.ShapeDtypeStruct((8, 128), f32),
                jax.ShapeDtypeStruct((2 * NL, 96, F), f32),
                jax.ShapeDtypeStruct((2 * NL, 96, F), f32),
                jax.ShapeDtypeStruct((NL, 8, PR, F), f32),
            ),
            in_specs=[anyspec] * 4,
            out_specs=(pl.BlockSpec(memory_space=pltpu.VMEM), anyspec, anyspec, anyspec),
            scratch_shapes=[
                V((NL, D, F), bf16), V((NL, F, D), bf16),
                V((8, PR, D), bf16), V((8, PR, D), bf16),
                V((NL, DS, F), f32), V((NL, DS, F), f32),
                V((2, PR, F), f32), V((PR, F), bf16), V((PR, F), bf16),
                V((NL, 8, DS, PR), bf16), V((PR, D), bf16), V((PR, D), bf16),
                V((2, PR, D), bf16), V((2, PR, D), bf16),
                V((DS, D), bf16), V((8, 128), f32), V((4, 8, 128), f32), V((8, 128), f32),
                DMA((NL, 2)), DMA((16,)), DMA((8,)), DMA((2,)), DMA((4,)), DMA((2,)),
                DMA((4, 3)), DMA((2, 3)), DMA((4,)), DMA((2,)), DMA((1,)), DMA((3,)), DMA, DMA,
                DMA((2,)), DMA((2,)), DMA((NL, 2)), DMA((NL, 2)), DMA((NL, 2)),
            ],
            compiler_params=pltpu.CompilerParams(collective_id=0, has_side_effects=True, vmem_limit_bytes=67043328),
            name="stack_step",
        )(x, y, w_up, w_down)
        return loss[0, 0], g_up, jnp.swapaxes(g_down, 1, 2)

    return jax.shard_map(
        per_device,
        mesh=mesh,
        in_specs=(P("data", None, None), P("data", None, None), P("stage", None, None), P("stage", None, None)),
        out_specs=(P(), P("stage", "data", None), P("stage", None, "data")),
        check_vma=False,
    )
```

```python
import functools

import jax
import jax.numpy as jnp
from jax import lax
from jax.experimental import pallas as pl
from jax.experimental.pallas import tpu as pltpu
from jax.sharding import PartitionSpec as P

bf16, f32 = jnp.bfloat16, jnp.float32
MESH = pl.DeviceIdType.MESH
NT = (((1,), (1,)), ((), ()))
C0 = 0.7978845608028654
C1 = C0 * 0.044715
D, F = 768, 3072
CH, PR = 128, 256
NL = 3
DS = 192
FB = 768
BLOCKS = [i * FB for i in range(F // FB)]
NSTEP = 23


def nn(a, b):
    return jnp.dot(a, b, preferred_element_type=f32)


def nt(a, b):
    return lax.dot_general(a, b, NT, preferred_element_type=f32)


def gelu_and_slope(u):
    s = u * u
    t = jnp.tanh(u * (C0 + C1 * s))
    a = 1.0 + t
    g = (0.5 * u) * a
    return g, 0.5 * a + g * ((1.0 - t) * (C0 + (3.0 * C1) * s))


def kernel(inv_total, x_in, y_in, w_up, w_down,
           loss_out, out_up, out_down, s_hbm, g_hbm, q_hbm, wta, wtb, hx, ex,
           wa, wb, acc1, acc2, hs, es, sb, gb, qb, hT, eTs, hb, eb, eout, tgt, sel, ltile, lbuf, lmine,
           wsem, rsem, hrecv, erecv, trecv, lrecv, xsend, hfwd, efwd, hsend, esend, tsend, lsend, lchain_s, lchain_r,
           os_s, os_g, os_q, is_s, is_g, is_q, is_h, is_e, tr_q, tr_h, xo_s, xo_r, lo_s):
    s = lax.axis_index("stage")
    d = lax.axis_index("data")
    c = d % 2
    q = d // 2
    k = 2 * s + c
    nxt = (s + c, d + 1 - 2 * c)
    prv = (s - 1 + c, d + 1 - 2 * c)
    partner = (s, d + 1 - 2 * c)
    peers = [(s, ((q + p) % 4) * 2 + c) for p in (1, 2, 3)]

    def rcopy(src, dst, ss, rs, dev):
        return pltpu.make_async_remote_copy(src_ref=src, dst_ref=dst, send_sem=ss, recv_sem=rs, device_id=dev, device_id_type=MESH)

    lcopy = pltpu.make_async_copy

    bar = pltpu.get_barrier_semaphore()
    for dev in peers:
        pl.semaphore_signal(bar, inc=1, device_id=dev, device_id_type=MESH)

    @pl.when(k < 7)
    def _():
        pl.semaphore_signal(bar, inc=1, device_id=nxt, device_id_type=MESH)

    @pl.when(k > 0)
    def _():
        pl.semaphore_signal(bar, inc=1, device_id=prv, device_id_type=MESH)

    def w_load(l):
        return (lcopy(w_up.at[NL * c + l], wa.at[l], wsem.at[l, 0]),
                lcopy(w_down.at[NL * c + l], wb.at[l], wsem.at[l, 1]))

    def w_reload(l):
        return (lcopy(wta.at[l], wa.at[l], rsem.at[l, 0]),
                lcopy(wtb.at[l], wb.at[l], rsem.at[l, 1]))

    def start_all(cps):
        for cp in cps:
            cp.start()

    def wait_all(cps):
        for cp in cps:
            cp.wait()

    for l in range(NL):
        start_all(w_load(l))

    def half(ch):
        return pl.ds(pl.multiple_of((ch % 2) * CH, CH), CH)

    def own(ref, j):
        return ref.at[j // 2, half(j), :]

    own0 = 4 * q

    @pl.when(k == 0)
    def _():
        for j in range(2):
            lcopy(x_in.at[pl.ds(j * CH, CH), :], own(hs, j), hrecv.at[own0 + j]).start()

    @pl.when(k == 7)
    def _():
        lcopy(y_in, tgt.at[1], trecv.at[1]).start()

    row = lax.broadcasted_iota(jnp.int32, (DS, D), 0)
    col = lax.broadcasted_iota(jnp.int32, (DS, D), 1)
    sel[...] = jnp.where(col == row + DS * q, 1.0, 0.0).astype(bf16)
    ltile[...] = jnp.zeros_like(ltile)

    pl.semaphore_wait(bar, 3 + jnp.where(k < 7, 1, 0) + jnp.where(k > 0, 1, 0))

    def xcopy(j):
        return rcopy(x_in.at[pl.ds(j * CH, CH), :], own(hs, 2 + j), xsend.at[j], hrecv.at[own0 + 2 + j], partner)

    def tcopy():
        return rcopy(y_in, tgt.at[0], tsend.at[0], trecv.at[0], partner)

    @pl.when(k == 1)
    def _():
        xcopy(0).start()
        xcopy(1).start()

    @pl.when(k == 6)
    def _():
        tcopy().start()

    def h_fwd(j, p):
        ch = own0 + j
        return rcopy(own(hs, j), hx.at[ch // 2, half(ch), :], hfwd.at[j, p], hrecv.at[ch], peers[p])

    def e_fwd(j, p):
        ch = own0 + j
        return rcopy(own(es, j), ex.at[ch // 2, half(ch), :], efwd.at[j, p], erecv.at[ch], peers[p])

    def h_out(j):
        return rcopy(own(tgt, j), own(hs, j), hsend.at[j], hrecv.at[own0 + j], nxt)

    def e_out(j):
        return rcopy(own(eout, j), own(es, j), esend.at[j], erecv.at[own0 + j], prv)

    def l_peer(p):
        return rcopy(lmine, lbuf.at[q], lsend.at[p], lrecv.at[q], peers[p])

    def l_chain():
        return rcopy(loss_out, loss_out, lchain_s, lchain_r, prv)

    def wait_chunk(buf, sems, ch):
        rcopy(own(buf, 0), own(buf, 0), hfwd.at[0, 0], sems.at[ch], peers[0]).wait_recv()

    def s_out_own(l, ch, b):
        return lcopy(sb.at[b, pl.ds(0, CH), :], s_hbm.at[l, ch // 2, half(ch), :], os_s.at[b])

    def g_out_own(l, ch, b):
        return lcopy(gb.at[b, pl.ds(0, CH), :], g_hbm.at[l, ch // 2, half(ch), :], os_g.at[b])

    def q_out_own(l, j, b):
        return lcopy(qb.at[b, pl.ds(0, CH), :], q_hbm.at[l, j // 2, half(j), :], os_q.at[b])

    def f_outs(l, pr, b):
        return lcopy(sb.at[b], s_hbm.at[l, pr], os_s.at[b]), lcopy(gb.at[b], g_hbm.at[l, pr], os_g.at[b])

    def s_in_own(l, ch, b):
        return lcopy(s_hbm.at[l, ch // 2, half(ch), :], sb.at[b, pl.ds(0, CH), :], is_s.at[b])

    def b_ins(l, pr, b):
        return lcopy(s_hbm.at[l, pr], sb.at[b], is_s.at[b]), lcopy(g_hbm.at[l, pr], gb.at[b], is_g.at[b])

    def w_ins(l, jp, b):
        return lcopy(q_hbm.at[l, jp], qb.at[b], is_q.at[b]), lcopy(g_hbm.at[l, 2 * q + jp], gb.at[b], is_g.at[b])

    def h_in(pr, b):
        return lcopy(hx.at[pr], hb.at[b], is_h.at[b])

    def e_in(pr, b):
        return lcopy(ex.at[pr], eb.at[b], is_e.at[b])

    high = k >= 4
    m = jnp.minimum(6, 2 * (7 - k))

    def is_tr(t):
        return t == jnp.where(high, 0, 4)

    def f_own_j(t):
        return jnp.where(high, t - 1, t)

    def is_f_own(t):
        return (t < 5) & jnp.logical_not(is_tr(t))

    def is_b_own(t):
        return (t >= 5 + m) & (t < 9 + m)

    def b_own_j(t):
        return t - 5 - m

    def is_w(t):
        return (t >= 9 + m) & (t < 11 + m)

    def w_jp(t):
        return t - 9 - m

    def is_b_oth(t):
        return (t >= 17) & (t < NSTEP)

    def is_f_oth(t):
        return ((t >= 5) & (t < 5 + m)) | ((t >= 11 + m) & (t < 17))

    def oth_pair(i):
        return 2 * ((q + 1 + i % 3) % 4) + i // 3

    def f_pair(t):
        return oth_pair(jnp.where(t < 5 + m, t - 5, t - 11))

    def b_pair(t):
        return oth_pair(t - 17)

    def is_loader(t):
        return is_b_own(t) | is_w(t) | is_b_oth(t)

    def start_load(t, li, b):
        l = 2 - li

        @pl.when(is_b_own(t))
        def _():
            s_in_own(l, own0 + b_own_j(t), b).start()

        @pl.when(is_w(t))
        def _():
            start_all(w_ins(l, w_jp(t), b))

        @pl.when(is_b_oth(t))
        def _():
            start_all(b_ins(l, b_pair(t), b))

    def next_load(t, li, b):
        @pl.when(li < 2)
        def _():
            start_load(t, li + 1, 1 - b)

        @pl.when(li == 2)
        def _():
            start_load(t + 1, 0, 1 - b)

    def first_load(t):
        @pl.when(is_f_oth(t - 1))
        def _():
            wait_all(f_outs(2, 0, (t + 1) % 2))

        @pl.when(jnp.logical_not(is_loader(t - 1)))
        def _():
            start_load(t, 0, t % 2)

    def pre_h(t):
        @pl.when(is_f_oth(t + 1))
        def _():
            pr = f_pair(t + 1)
            wait_chunk(hs, hrecv, 2 * pr)
            wait_chunk(hs, hrecv, 2 * pr + 1)
            h_in(pr, (t + 1) % 2).start()

    def pre_e(t):
        @pl.when(is_b_oth(t + 1))
        def _():
            pr = b_pair(t + 1)
            wait_chunk(es, erecv, 2 * pr)
            wait_chunk(es, erecv, 2 * pr + 1)
            e_in(pr, (t + 1) % 2).start()

    def wait_reload(t, l):
        @pl.when(t == 5)
        def _():
            wait_all(w_reload(l))

    def tr_step(t):
        def zero(i, carry):
            r = pl.ds(pl.multiple_of(i * 8, 8), 8)
            for l in range(NL):
                acc1[l, r, :] = jnp.zeros((8, F), f32)
                acc2[l, r, :] = jnp.zeros((8, F), f32)
            return carry

        lax.fori_loop(0, DS // 8, zero, 0)

        def layer(l, carry):
            @pl.when(high)
            def _():
                wait_all(w_load(l))

            stage = [hb.at[0], hb.at[1], eb.at[0], eb.at[1]]
            pend_q, pend_h = [None] * 2, [None] * 4
            for i in range(3):
                if pend_q[i % 2] is not None:
                    pend_q[i % 2].wait()
                qb[i % 2] = wb[l, :, i * 256:(i + 1) * 256].T
                pend_q[i % 2] = lcopy(qb.at[i % 2], wta.at[l, pl.ds(i * 256, 256), :], tr_q.at[i % 2])
                pend_q[i % 2].start()
                for r in range(4 * i, 4 * i + 4):
                    if pend_h[r % 4] is not None:
                        pend_h[r % 4].wait()
                    stage[r % 4][...] = wa[l, :, r * 256:(r + 1) * 256].T
                    pend_h[r % 4] = lcopy(stage[r % 4], wtb.at[l, pl.ds(r * 256, 256), :], tr_h.at[r % 4])
                    pend_h[r % 4].start()
            wait_all(pend_q + pend_h)

            @pl.when(jnp.logical_not(high))
            def _():
                start_all(w_reload(l))

            return carry

        lax.fori_loop(0, NL, layer, 0)
        pre_h(t)

    def f_own(t):
        j = f_own_j(t)
        ch = own0 + j
        wait_chunk(hs, hrecv, ch)
        for p in range(3):
            h_fwd(j, p).start()
        pre_h(t)
        hb[0, 0:CH, :] = hs[j // 2, half(j), :]

        def layer(l, carry):
            b = l % 2

            @pl.when((j == 0) & jnp.logical_not(high))
            def _():
                wait_all(w_load(l))

            @pl.when(l == 2)
            def _():
                s_out_own(0, ch, 0).wait()
                g_out_own(0, ch, 0).wait()

            h = hb[0, 0:CH, :]
            hT[l, ch // 2, :, half(ch)] = nt(sel[...], h).astype(bf16)
            for o in BLOCKS:
                g, slope = gelu_and_slope(nn(h, wa[l, :, o:o + FB]))
                sb[b, 0:CH, o:o + FB] = slope
                gb[b, 0:CH, o:o + FB] = g.astype(bf16)
            hb[0, 0:CH, :] = (h.astype(f32) + nn(gb[b, 0:CH, :], wb[l])).astype(bf16)
            s_out_own(l, ch, b).start()
            g_out_own(l, ch, b).start()

            @pl.when((j == 3) & high)
            def _():
                start_all(w_reload(l))

            return carry

        lax.fori_loop(0, NL, layer, 0)

        @pl.when(k < 7)
        def _():
            tgt[j // 2, half(j), :] = hb[0, 0:CH, :]
            h_out(j).start()

        @pl.when(k == 7)
        def _():
            @pl.when(j == 0)
            def _():
                rcopy(y_in, tgt.at[0], tsend.at[0], trecv.at[0], partner).wait_recv()

            @pl.when(j == 2)
            def _():
                lcopy(y_in, tgt.at[1], trecv.at[1]).wait()

            diff = hb[0, 0:CH, :].astype(f32) - tgt[j // 2, half(j), :].astype(f32)
            es[j // 2, half(j), :] = (diff * inv_total).astype(bf16)
            sq = jnp.sum((diff * diff).reshape(CH // 8, 8, D), axis=0)
            ltile[...] += sum(sq[:, i * 128:(i + 1) * 128] for i in range(D // 128))

            @pl.when(j == 3)
            def _():
                lmine[...] = ltile[...]

        s_out_own(1, ch, 1).wait()
        g_out_own(1, ch, 1).wait()
        s_out_own(2, ch, 0).wait()
        g_out_own(2, ch, 0).wait()

    def f_oth(t):
        pr = f_pair(t)
        hi = t % 2
        h_in(pr, hi).wait()

        def layer(l, carry):
            b = (t + l) % 2
            wait_reload(t, l)

            @pl.when((l == 1) & is_f_oth(t - 1))
            def _():
                wait_all(f_outs(2, 0, b))

            @pl.when(l == 1)
            def _():
                pre_h(t)
                pre_e(t)

            @pl.when(l == 2)
            def _():
                wait_all(f_outs(0, pr, b))

            h = hb[hi]
            hT[l, pr] = nt(sel[...], h).astype(bf16)
            for o in BLOCKS:
                g, slope = gelu_and_slope(nt(h, wb[l, o:o + FB, :]))
                sb[b, :, o:o + FB] = slope
                gb[b, :, o:o + FB] = g.astype(bf16)
            start_all(f_outs(l, pr, b))

            @pl.when(l < 2)
            def _():
                hb[hi] = (hb[hi].astype(f32) + nt(gb[b], wa[l])).astype(bf16)

            return carry

        lax.fori_loop(0, NL, layer, 0)
        wait_all(f_outs(1, pr, (t + 1) % 2))

    def b_own(t):
        j = b_own_j(t)
        ch = own0 + j
        jp = j // 2
        first_load(t)

        @pl.when(k < 7)
        def _():
            wait_chunk(es, erecv, ch)

        for p in range(3):
            e_fwd(j, p).start()
        eb[0, 0:CH, :] = es[jp, half(j), :]

        def layer(li, carry):
            l = 2 - li
            b = (t + li) % 2
            s_in_own(l, ch, b).wait()

            @pl.when(li == 2)
            def _():
                q_out_own(2, j, b).wait()
                q_out_own(1, j, 1 - b).wait()

            next_load(t, li, b)
            wait_reload(t, l)
            e = eb[0, 0:CH, :]
            eTs[jp, l, :, half(j)] = nt(sel[...], e).astype(bf16)
            for o in BLOCKS:
                p = nn(e, wa[l, :, o:o + FB]).astype(bf16).astype(f32)
                qb[b, 0:CH, o:o + FB] = (p * sb[b, 0:CH, o:o + FB]).astype(bf16)
            eb[0, 0:CH, :] = (e.astype(f32) + nn(qb[b, 0:CH, :], wb[l])).astype(bf16)
            q_out_own(l, j, b).start()
            return carry

        lax.fori_loop(0, NL, layer, 0)

        @pl.when(k > 0)
        def _():
            eout[jp, half(j), :] = eb[0, 0:CH, :]
            e_out(j).start()

        q_out_own(0, j, t % 2).wait()

    def wgrad(l, hTl, eTl, b):
        for o in BLOCKS:
            acc1[l, :, o:o + FB] += nn(hTl, qb[b, :, o:o + FB])
            acc2[l, :, o:o + FB] += nn(eTl, gb[b, :, o:o + FB])

    def w_step(t):
        jp = w_jp(t)

        def layer(li, carry):
            l = 2 - li
            b = (t + li) % 2
            wait_all(w_ins(l, jp, b))
            next_load(t, li, b)

            @pl.when(li == 1)
            def _():
                pre_h(t)
                pre_e(t)

            wgrad(l, hT[l, 2 * q + jp], eTs[jp, l], b)
            return carry

        lax.fori_loop(0, NL, layer, 0)

        @pl.when(jp == 1)
        def _():
            @pl.when(k == 7)
            def _():
                for p in range(3):
                    l_peer(p).start()
                for p in range(3):
                    qo = (q + 1 + p) % 4
                    rcopy(lmine, lbuf.at[qo], lsend.at[p], lrecv.at[qo], peers[p]).wait_recv()
                lbuf[q] = lmine[...]
                tot = (lbuf[0] + lbuf[1]) + (lbuf[2] + lbuf[3])
                loss_out[...] = jnp.zeros((8, 128), f32) + jnp.sum(tot) * (0.5 * inv_total)

            @pl.when(k < 7)
            def _():
                l_chain().wait_recv()

            @pl.when(k > 0)
            def _():
                l_chain().start()

    half_own = pl.ds(pl.multiple_of(96 * c, 8), 96)
    half_oth = pl.ds(pl.multiple_of(96 * (1 - c), 8), 96)

    def final_copies(l):
        lg = NL * c + l
        return [
            rcopy(acc1.at[l, half_oth, :], out_up.at[lg], xo_s.at[l, 0], xo_r.at[l, 0], partner),
            rcopy(acc2.at[l, half_oth, :], out_down.at[lg], xo_s.at[l, 1], xo_r.at[l, 1], partner),
            lcopy(acc1.at[l, half_own, :], out_up.at[lg], lo_s.at[l, 0]),
            lcopy(acc2.at[l, half_own, :], out_down.at[lg], lo_s.at[l, 1]),
        ]

    def b_oth(t):
        pr = b_pair(t)
        ei = t % 2
        first_load(t)
        e_in(pr, ei).wait()

        def layer(li, carry):
            l = 2 - li
            b = (t + li) % 2
            wait_all(b_ins(l, pr, b))
            next_load(t, li, b)

            @pl.when(li == 1)
            def _():
                pre_e(t)

            e = eb[ei]
            eT = nt(sel[...], e).astype(bf16)
            for o in BLOCKS:
                p = nn(e, wa[l, :, o:o + FB]).astype(bf16).astype(f32)
                qb[b, :, o:o + FB] = (p * sb[b, :, o:o + FB]).astype(bf16)
            wgrad(l, hT[l, pr], eT, b)

            @pl.when(l > 0)
            def _():
                eb[ei] = (eb[ei].astype(f32) + nn(qb[b], wb[l])).astype(bf16)

            @pl.when(t == NSTEP - 1)
            def _():
                start_all(final_copies(l))

            return carry

        lax.fori_loop(0, NL, layer, 0)

    def step(t, carry):
        for test, run in ((is_tr, tr_step), (is_f_own, f_own), (is_f_oth, f_oth), (is_b_own, b_own), (is_w, w_step), (is_b_oth, b_oth)):
            @pl.when(test(t))
            def _():
                run(t)

        return carry

    lax.fori_loop(0, NSTEP, step, 0)

    for j in range(4):
        for p in range(3):
            h_fwd(j, p).wait_send()
            e_fwd(j, p).wait_send()

    @pl.when(k < 7)
    def _():
        for j in range(4):
            h_out(j).wait_send()

    @pl.when(k > 0)
    def _():
        for j in range(4):
            e_out(j).wait_send()
        l_chain().wait_send()

    @pl.when(k == 1)
    def _():
        xcopy(0).wait_send()
        xcopy(1).wait_send()

    @pl.when(k == 6)
    def _():
        tcopy().wait_send()

    @pl.when(k == 7)
    def _():
        for p in range(3):
            l_peer(p).wait_send()

    for l in range(NL):
        lg = NL * (1 - c) + l
        rcopy(acc1.at[l, half_oth, :], out_up.at[lg], xo_s.at[l, 0], xo_r.at[l, 0], partner).wait_recv()
        rcopy(acc2.at[l, half_oth, :], out_down.at[lg], xo_s.at[l, 1], xo_r.at[l, 1], partner).wait_recv()
        r1, r2, l1, l2 = final_copies(l)
        r1.wait_send()
        r2.wait_send()
        l1.wait()
        l2.wait()


def solution(mesh):
    n_data = mesh.shape["data"]

    def per_device(inputs, targets, w_up, w_down):
        n_micro, n_tok, width = inputs.shape
        inv_total = 1.0 / (n_data * n_micro * n_tok)
        x = inputs.reshape(n_micro * n_tok, width)
        y = targets.reshape(n_micro * n_tok, width)
        V = pltpu.VMEM
        DMA = pltpu.SemaphoreType.DMA
        S = jax.ShapeDtypeStruct
        anyspec = pl.BlockSpec(memory_space=pl.ANY)
        outs = pl.pallas_call(
            functools.partial(kernel, inv_total),
            out_shape=(
                S((8, 128), f32), S((2 * NL, 96, F), f32), S((2 * NL, 96, F), f32),
                S((NL, 8, PR, F), f32), S((NL, 8, PR, F), bf16), S((NL, 2, PR, F), bf16),
                S((NL, D, F), bf16), S((NL, F, D), bf16), S((8, PR, D), bf16), S((8, PR, D), bf16),
            ),
            in_specs=[anyspec] * 4,
            out_specs=(pl.BlockSpec(memory_space=pltpu.VMEM),) + (anyspec,) * 9,
            scratch_shapes=[
                V((NL, D, F), bf16), V((NL, F, D), bf16),
                V((NL, DS, F), f32), V((NL, DS, F), f32),
                V((2, PR, D), bf16), V((2, PR, D), bf16),
                V((2, PR, F), f32), V((2, PR, F), bf16), V((2, PR, F), bf16),
                V((NL, 8, DS, PR), bf16), V((2, NL, DS, PR), bf16),
                V((2, PR, D), bf16), V((2, PR, D), bf16), V((2, PR, D), bf16), V((2, PR, D), bf16),
                V((DS, D), bf16), V((8, 128), f32), V((4, 8, 128), f32), V((8, 128), f32),
                DMA((NL, 2)), DMA((NL, 2)), DMA((16,)), DMA((16,)), DMA((2,)), DMA((4,)), DMA((2,)),
                DMA((4, 3)), DMA((4, 3)), DMA((4,)), DMA((4,)), DMA((1,)), DMA((3,)), DMA, DMA,
                DMA((2,)), DMA((2,)), DMA((2,)), DMA((2,)), DMA((2,)), DMA((2,)), DMA((2,)), DMA((2,)), DMA((2,)), DMA((4,)),
                DMA((NL, 2)), DMA((NL, 2)), DMA((NL, 2)),
            ],
            compiler_params=pltpu.CompilerParams(collective_id=0, has_side_effects=True, vmem_limit_bytes=67043328),
            name="stack_step",
        )(x, y, w_up, w_down)
        return outs[0][0, 0], outs[1], jnp.swapaxes(outs[2], 1, 2)

    return jax.shard_map(
        per_device,
        mesh=mesh,
        in_specs=(P("data", None, None), P("data", None, None), P("stage", None, None), P("stage", None, None)),
        out_specs=(P(), P("stage", "data", None), P("stage", None, "data")),
        check_vma=False,
    )
```

```python
import functools

import jax
import jax.numpy as jnp
from jax import lax
from jax.experimental import pallas as pl
from jax.experimental.pallas import tpu as pltpu
from jax.sharding import PartitionSpec as P

bf16, f32 = jnp.bfloat16, jnp.float32
MESH = pl.DeviceIdType.MESH
NT = (((1,), (1,)), ((), ()))
C0 = 0.7978845608028654
C1 = C0 * 0.044715
D, F = 768, 3072
CH, PR = 128, 256
NL = 3
DS = 192
FB, FW, DW = 512, 768, 256
BLOCKS = [i * FB for i in range(F // FB)]
NSTEP = 23
PER = 2
TOP = NL - 1
PEERS = range(3)
HEAD = slice(0, CH)


def each_layer(layer, peel=False):
    if peel:
        layer(0, 0)
    lax.fori_loop(int(peel), NL, layer, 0)


def flip(t):
    return (t + 1) % PER


def nn(a, b):
    return jnp.dot(a, b, preferred_element_type=f32)


def nt(a, b):
    return lax.dot_general(a, b, NT, preferred_element_type=f32)


def gelu_and_slope(u):
    s = u * u
    t = jnp.tanh(u * (C0 + C1 * s))
    a = 1.0 + t
    g = (0.5 * u) * a
    return g, 0.5 * a + g * ((1.0 - t) * (C0 + (3.0 * C1) * s))


def two_matmuls(va, first, second):
    v = first(BLOCKS[0])
    for o in BLOCKS[1:]:
        w = first(o)
        va[...] += second(o - FB, v)
        v = w
    return va[...] + second(BLOCKS[-1], v)


def kernel(inv_total, x_in, y_in, w_up, w_down,
           loss_out, out_up, out_down, s_hbm, g_hbm, q_hbm, wta, wtb, hx, ex, hx2, ex1,
           wa, wb, acc1, acc2, hs, es, sb, gb, qb, hT, eTs, hb, eb, eout, tgt, sv, va, sel, ltile, lbuf, lmine,
           wsem, rsem, h2recv, e1recv, h2fwd, e1fwd, is_x, os_x, hrecv, erecv, trecv, lrecv, xsend, hfwd, efwd, hsend, esend, tsend, lsend, lout_s, lout_r,
           os_s, os_g, os_q, is_s, is_g, is_q, is_h, is_e, tr_q, tr_h, xo_s, xo_r, lo_s):
    s = lax.axis_index("stage")
    d = lax.axis_index("data")
    c = d % PER
    q = d // PER
    k = PER * s + c
    nxt = (s + c, d + 1 - PER * c)
    prv = (s - 1 + c, d + 1 - PER * c)
    partner = (s, d + 1 - PER * c)
    peers = [(s, ((q + p) % 4) * 2 + c) for p in (1, 2, 3)]

    def rcopy(src, dst, ss, rs, dev):
        return pltpu.make_async_remote_copy(src_ref=src, dst_ref=dst, send_sem=ss, recv_sem=rs, device_id=dev, device_id_type=MESH)

    lcopy = pltpu.make_async_copy
    hc = hb.at[0, HEAD, :]
    ec = eb.at[0, HEAD, :]

    bar = pltpu.get_barrier_semaphore()
    for dev in peers:
        pl.semaphore_signal(bar, inc=1, device_id=dev, device_id_type=MESH)

    @pl.when(k < 7)
    def _():
        pl.semaphore_signal(bar, inc=1, device_id=nxt, device_id_type=MESH)

    @pl.when(k > 0)
    def _():
        pl.semaphore_signal(bar, inc=1, device_id=prv, device_id_type=MESH)

    @pl.when(k < 6)
    def _():
        pl.semaphore_signal(bar, inc=1, device_id=(3, PER * q + 1), device_id_type=MESH)

    def w_load(l):
        return (lcopy(w_up.at[NL * c + l], wa.at[l], wsem.at[l, 0]),
                lcopy(w_down.at[NL * c + l], wb.at[l], wsem.at[l, 1]))

    def w_reload(l):
        return (lcopy(wta.at[l], wa.at[l], rsem.at[l, 0]),
                lcopy(wtb.at[l], wb.at[l], rsem.at[l, 1]))

    def start_all(cps):
        for cp in cps:
            cp.start()

    def wait_all(cps):
        for cp in cps:
            cp.wait()

    def half(ch):
        return pl.ds(pl.multiple_of((ch % PER) * CH, CH), CH)

    def own(ref, j):
        return ref.at[j // PER, half(j), :]

    own0 = 4 * q

    @pl.when(k == 0)
    def _():
        for j in range(2):
            lcopy(x_in.at[pl.ds(j * CH, CH), :], own(hs, j), hrecv.at[own0 + j]).start()

    for l in range(NL):
        start_all(w_load(l))

    @pl.when(k == 7)
    def _():
        lcopy(y_in, tgt.at[1], trecv.at[1]).start()

    row = lax.broadcasted_iota(jnp.int32, (DS, D), 0)
    col = lax.broadcasted_iota(jnp.int32, (DS, D), 1)
    sel[...] = jnp.where(col == row + DS * q, 1.0, 0.0).astype(bf16)
    ltile[...] = jnp.zeros_like(ltile)

    pl.semaphore_wait(bar, 3 + jnp.where(k < 7, 1, 7) + jnp.where((k > 0) & (k < 7), 1, 0))

    def xcopy(j):
        return rcopy(x_in.at[pl.ds(j * CH, CH), :], own(hs, 2 + j), xsend.at[j], hrecv.at[own0 + 2 + j], partner)

    def tcopy():
        return rcopy(y_in, tgt.at[0], tsend.at[0], trecv.at[0], partner)

    @pl.when(k == 1)
    def _():
        xcopy(0).start()
        xcopy(1).start()

    @pl.when(k == 6)
    def _():
        tcopy().start()

    def h_fwd(j, p):
        ch = own0 + j
        return rcopy(own(hs, j), hx.at[ch // PER, half(ch), :], hfwd.at[j, p], hrecv.at[ch], peers[p])

    def e_fwd(j, p):
        ch = own0 + j
        return rcopy(own(es, j), ex.at[ch // PER, half(ch), :], efwd.at[j, p], erecv.at[ch], peers[p])

    def h2_fwd(j, p):
        ch = own0 + j
        at = hx2.at[ch // PER, half(ch), :]
        return rcopy(at, at, h2fwd.at[j, p], h2recv.at[ch], peers[p])

    def e1_fwd(j, p):
        ch = own0 + j
        at = ex1.at[ch // PER, half(ch), :]
        return rcopy(at, at, e1fwd.at[j, p], e1recv.at[ch], peers[p])

    def h2_save(j):
        ch = own0 + j
        return lcopy(sv.at[1], hx2.at[ch // PER, half(ch), :], os_x.at[0])

    def e1_save(j, b):
        ch = own0 + j
        return lcopy(sv.at[b], ex1.at[ch // PER, half(ch), :], os_x.at[b])

    def h_out(j):
        return rcopy(own(tgt, j), own(hs, j), hsend.at[j], hrecv.at[own0 + j], nxt)

    def e_out(j):
        return rcopy(eout.at[half(j), :], own(es, j), esend.at[j], erecv.at[own0 + j], prv)

    def l_peer(p):
        return rcopy(lmine, lbuf.at[q], lsend.at[p], lrecv.at[q], peers[p])

    def l_out(kk):
        return rcopy(loss_out, loss_out, lout_s.at[kk], lout_r, (kk // PER, PER * q + kk % PER))

    def wait_chunk(buf, sems, ch):
        rcopy(own(buf, 0), own(buf, 0), hfwd.at[0, 0], sems.at[ch], peers[0]).wait_recv()

    def s_out_own(l, ch, b):
        return lcopy(sb.at[b, half(ch), :], s_hbm.at[l, ch // PER, half(ch), :], os_s.at[b])

    def g_out_own(l, ch, b):
        return lcopy(gb.at[b, half(ch), :], g_hbm.at[l, ch // PER, half(ch), :], os_g.at[b])

    def q_out_own(l, j, b):
        return lcopy(qb.at[b, HEAD, :], q_hbm.at[l, j // PER, half(j), :], os_q.at[b])

    def f_drain(b):
        s_out_own(0, 0, b).wait()
        g_out_own(0, 0, b).wait()

    def f_drain_all():
        for b in range(PER):
            f_drain(b)

    def f_outs(l, pr, b):
        return lcopy(sb.at[b], s_hbm.at[l, pr], os_s.at[b]), lcopy(gb.at[b], g_hbm.at[l, pr], os_g.at[b])

    def s_in_own(l, ch, b):
        return lcopy(s_hbm.at[l, ch // PER, half(ch), :], sb.at[b, HEAD, :], is_s.at[b])

    def b_ins(l, pr, b):
        return lcopy(s_hbm.at[l, pr], sb.at[b], is_s.at[b]), lcopy(g_hbm.at[l, pr], gb.at[b], is_g.at[b])

    def w_ins(l, jp, b):
        return lcopy(q_hbm.at[l, jp], qb.at[b], is_q.at[b]), lcopy(g_hbm.at[l, PER * q + jp], gb.at[b], is_g.at[b])

    def h_in(pr, b):
        return lcopy(hx.at[pr], hb.at[b], is_h.at[b])

    def e_in(pr, b):
        return lcopy(ex.at[pr], eb.at[b], is_e.at[b])

    def h2_in(pr, b):
        return lcopy(hx2.at[pr], tgt.at[b], is_x.at[b])

    def e1_in(pr, b):
        return lcopy(ex1.at[pr], tgt.at[b], is_x.at[b])

    def wait_pair(sems, pr):
        wait_chunk(hs, sems, PER * pr)
        wait_chunk(hs, sems, PER * pr + 1)

    first, last = k == 0, k == 7
    mid = (k > 0) & (k < 7)
    high = k >= 4

    def flag(x):
        return jnp.where(x, 1, 0)

    m = 6 * flag(k < 3) + 4 * flag(k == 3) + 3 * flag(k == 4) + 2 * flag(k == 5)
    end = jnp.where(mid, 22, 18)

    def within(t, a, b):
        return (t >= a) & (t < b)

    def is_tr(t):
        return t == jnp.where(high, 0, 4)

    def is_bx(t):
        return last & ((t == 3) | (t == 6))

    def bx_jp(t):
        return t // 6

    def is_f_own(t):
        return within(t, 0, jnp.where(last, 6, 5)) & jnp.logical_not(is_tr(t) | is_bx(t))

    def f_own_j(t):
        return jnp.where(high, t - 1, t) - flag(last & (t > 3))

    def is_b_own(t):
        return mid & (within(t, 5 + m, 7 + m) | within(t, 8 + m, 10 + m))

    def b_own_j(t):
        return t - 5 - m - flag(t > 7 + m)

    def is_w(t):
        return mid & (within(t, jnp.where(high, 15, 10 + m), jnp.where(high, 17, 11 + m)) | (is_gap(t) & jnp.logical_not(high)))

    def w_jp(t):
        return jnp.where(high, t - 15, flag(t > 7 + m))

    def is_ob(t):
        return first & ((t == 11) | (t == 14))

    def ob_jp(t):
        return t // 14

    def is_gap(t):
        return mid & (t == 7 + m)

    def is_b_oth(t):
        return (mid & within(t, 17, 23)) | (first & within(t, 11, 19)) | (last & within(t, 13, 19))

    def is_f_oth(t):
        return (first & within(t, 5, 11)) | (last & within(t, 7, 13)) | (is_gap(t) & high) | (mid & (within(t, 5, 5 + m) | within(t, jnp.where(high, 10, 11) + m, jnp.where(high, 15, 17))))

    def oth_pair(i):
        return 2 * ((q + 1 + i % 3) % 4) + i // 3

    def f_pair(t):
        i = jnp.where(t < 5 + m, t - 5, jnp.where(is_gap(t), m, jnp.where(high, t - 9, t - 11)))
        return oth_pair(jnp.where(last, t - 7, i))

    def b_pair(t):
        i0 = jnp.where(t < 14, t - 12, t - 13)
        i = jnp.where(first, i0, jnp.where(last, t - 13, t - 17))
        return jnp.where(is_ob(t), PER * q + ob_jp(t), oth_pair(jnp.maximum(i, 0)))

    def is_loader(t):
        return is_b_own(t) | is_w(t) | is_b_oth(t)

    def start_load(t, li, b):
        l = TOP - li

        @pl.when(is_b_own(t))
        def _():
            s_in_own(l, own0 + b_own_j(t), b).start()

        @pl.when(is_w(t))
        def _():
            start_all(w_ins(l, w_jp(t), b))

        @pl.when(is_b_oth(t))
        def _():
            start_all(b_ins(l, b_pair(t), b))

    def next_load(t, li, b):
        @pl.when(li < 2)
        def _():
            start_load(t, li + 1, 1 - b)

        @pl.when(li == TOP)
        def _():
            start_load(t + 1, 0, 1 - b)

    def first_load(t):
        @pl.when(is_f_oth(t - 1))
        def _():
            wait_all(f_outs(2, 0, flip(t)))

        @pl.when(is_f_own(t - 1))
        def _():
            f_drain_all()

        @pl.when(jnp.logical_not(is_loader(t - 1) | is_f_oth(t - 1) | is_f_own(t - 1)))
        def _():
            start_load(t, 0, t % PER)

    def pre_h(t):
        @pl.when(is_f_oth(t + 1))
        def _():
            pr = f_pair(t + 1)
            wait_chunk(hs, hrecv, PER * pr)
            wait_chunk(hs, hrecv, PER * pr + 1)
            h_in(pr, flip(t)).start()

    def pre_e(t):
        @pl.when(is_b_oth(t + 1) & jnp.logical_not(is_ob(t + 1)))
        def _():
            pr = b_pair(t + 1)
            wait_chunk(es, erecv, PER * pr)
            wait_chunk(es, erecv, PER * pr + 1)
            e_in(pr, flip(t)).start()

    def wait_reload(t, l):
        @pl.when(t == jnp.where(last, 7, 5))
        def _():
            wait_all(w_reload(l))

    def tr_step(t):
        def zero(i, carry):
            r = pl.ds(pl.multiple_of(i * 8, 8), 8)
            for l in range(NL):
                acc1[l, r, :] = jnp.zeros((8, F), f32)
                acc2[l, r, :] = jnp.zeros((8, F), f32)
            return carry

        lax.fori_loop(0, DS // 8, zero, 0)

        @pl.when(jnp.logical_not(high))
        def _():
            f_drain_all()

        stage = [hb.at[0], hb.at[1], eb.at[0], eb.at[1], eout]
        pend_q, pend_h = [None] * 2, [None] * 5

        def reload(l):
            @pl.when(jnp.logical_not(high))
            def _():
                start_all(w_reload(l))

        def put(pend, sems, n, buf, src, dst):
            if pend[n] is not None:
                pend[n].wait()
            for o in range(0, src.shape[0], D):
                buf[:, o:o + D] = src[o:o + D, :].T
            pend[n] = lcopy(buf, dst, sems.at[n])
            pend[n].start()

        for l in range(NL):
            @pl.when(high)
            def _():
                wait_all(w_load(l))

            for i in range(3):
                put(pend_q, tr_q, i % PER, qb.at[i % PER], wb.at[l, :, pl.ds(i * 256, 256)], wta.at[l, pl.ds(i * 256, 256), :])
                for r in range(4 * i, 4 * i + 4):
                    put(pend_h, tr_h, r % 5, stage[r % 5], wa.at[l, :, pl.ds(r * 256, 256)], wtb.at[l, pl.ds(r * 256, 256), :])
            if l > 0:
                reload(l - 1)
        wait_all(pend_q + pend_h)
        reload(NL - 1)
        pre_h(t)

    def f_own(t):
        j = f_own_j(t)
        ch = own0 + j
        rows = half(j)
        wait_chunk(hs, hrecv, ch)
        for p in PEERS:
            h_fwd(j, p).start()
        hc[...] = hs[j // PER, rows, :]

        def layer(l, carry):
            b = l % PER

            @pl.when((j == 0) & jnp.logical_not(high))
            def _():
                wait_all(w_load(l))

            @pl.when((l == TOP) | is_f_own(t - 1))
            def _():
                f_drain(b)

            @pl.when((k == 6) & (j == 3) & (l == 1))
            def _():
                start_load(t + 1, 0, flip(t))

            h = hc[...]

            sv[jnp.maximum(l - 1, 0)] = h
            acc = va.at[HEAD, :]
            acc[...] = h.astype(f32)

            def up(o):
                g, slope = gelu_and_slope(nn(h, wa[l, :, o:o + FB]))
                sb[b, rows, o:o + FB] = slope
                g = g.astype(bf16)
                gb[b, rows, o:o + FB] = g
                return g

            hc[...] = two_matmuls(acc, up, lambda o, g: nn(g, wb[l, o:o + FB, :])).astype(bf16)
            s_out_own(l, ch, b).start()
            g_out_own(l, ch, b).start()

            @pl.when((j == 3) & within(k, 4, 7))
            def _():
                start_all(w_reload(l))

            return carry

        each_layer(layer)

        @pl.when(k < 7)
        def _():
            tgt[j // PER, rows, :] = hc[...]
            h_out(j).start()

        @pl.when(k == 7)
        def _():
            @pl.when(j == 0)
            def _():
                rcopy(y_in, tgt.at[0], tsend.at[0], trecv.at[0], partner).wait_recv()

            @pl.when(j == 2)
            def _():
                lcopy(y_in, tgt.at[1], trecv.at[1]).wait()

            diff = hc[...].astype(f32) - tgt[j // PER, rows, :].astype(f32)
            es[j // PER, rows, :] = (diff * inv_total).astype(bf16)
            sq = jnp.sum((diff * diff).reshape(CH // 8, 8, D), axis=0)
            ltile[...] += sum(sq[:, i * 128:(i + 1) * 128] for i in range(D // 128))

            @pl.when(j == 3)
            def _():
                lmine[...] = ltile[...]

        h2_save(j).start()
        hT[0, ch // PER, :, rows] = nt(sel[...], hs[j // PER, rows, :]).astype(bf16)
        for l in range(1, NL):
            hT[l, ch // PER, :, rows] = nt(sel[...], sv[l - 1]).astype(bf16)
        h2_save(j).wait()
        for p in PEERS:
            h2_fwd(j, p).start()
        pre_h(t)

    def q_drain(t, li):
        @pl.when((li == flag(is_b_own(t))) & is_b_own(t - 1))
        def _():
            q_out_own(0, 0, flip(t)).wait()

    def f_oth(t):
        pr = f_pair(t)
        hi = t % PER

        @pl.when(is_f_own(t - 1))
        def _():
            f_drain_all()

        q_drain(t, 0)

        @pl.when((k < 7) & (t == 5 + 2 * flag(k == 6)))
        def _():
            for j in range(4):
                h_out(j).wait_send()

        h_in(pr, hi).wait()

        def layer(l, carry):
            b = (t + l) % PER
            wait_reload(t, l)

            if not isinstance(l, int):
                @pl.when((l == 1) & is_f_oth(t - 1))
                def _():
                    wait_all(f_outs(2, 0, b))

                @pl.when(l == 1)
                def _():
                    wait_pair(h2recv, pr)
                    h2_in(pr, hi).start()
                    pre_h(t)
                    pre_e(t)

                @pl.when(l == TOP)
                def _():
                    wait_all(f_outs(0, pr, b))
                    h2_in(pr, hi).wait()
                    hb[hi] = tgt[hi]

            h = hb[hi]
            hT[l, pr] = nt(sel[...], h).astype(bf16)

            def up(o):
                g, slope = gelu_and_slope(nt(h, wb[l, o:o + FB, :]))
                sb[b, :, o:o + FB] = slope
                g = g.astype(bf16)
                gb[b, :, o:o + FB] = g
                return g

            if isinstance(l, int):
                va[...] = h.astype(f32)
                hb[hi] = two_matmuls(va, up, lambda o, g: nt(g, wa[l, :, o:o + FB])).astype(bf16)
            else:
                for o in BLOCKS:
                    up(o)
            start_all(f_outs(l, pr, b))
            return carry

        each_layer(layer, peel=True)
        wait_all(f_outs(1, pr, flip(t)))

        @pl.when(is_loader(t + 1))
        def _():
            start_load(t + 1, 0, flip(t))

    def b_own(t):
        j = b_own_j(t)
        ch = own0 + j
        jp = j // PER
        first_load(t)
        wait_chunk(es, erecv, ch)
        for p in PEERS:
            e_fwd(j, p).start()
        ec[...] = es[jp, half(j), :]

        def layer(li, carry):
            l = TOP - li
            b = (t + li) % PER
            s_in_own(l, ch, b).wait()
            q_drain(t, li)

            @pl.when(li == TOP)
            def _():
                q_out_own(2, j, b).wait()
                q_out_own(1, j, 1 - b).wait()

            next_load(t, li, b)
            wait_reload(t, l)
            e = ec[...]

            sv[jnp.maximum(li - 1, 0)] = e
            acc = va.at[HEAD, :]
            acc[...] = e.astype(f32)

            def up(o):
                p = nn(e, wa[l, :, o:o + FB]).astype(bf16).astype(f32)
                qv = (p * sb[b, HEAD, o:o + FB]).astype(bf16)
                qb[b, HEAD, o:o + FB] = qv
                return qv

            ec[...] = two_matmuls(acc, up, lambda o, qv: nn(qv, wb[l, o:o + FB, :])).astype(bf16)
            q_out_own(l, j, b).start()
            return carry

        each_layer(layer)
        @pl.when(j >= 2)
        def _():
            e_out(j - 2).wait_send()

        eout[half(j), :] = ec[...]
        e_out(j).start()
        e1_save(j, 1).start()
        eTs[jp, 2, :, half(j)] = nt(sel[...], es[jp, half(j), :]).astype(bf16)
        for li in range(1, NL):
            eTs[jp, TOP - li, :, half(j)] = nt(sel[...], sv[li - 1]).astype(bf16)
        e1_save(j, 1).wait()

        @pl.when(j == jnp.where(k > 1, 1, 2))
        def _():
            for i in range(2):
                for p in PEERS:
                    e1_fwd(i, p).start()

        @pl.when(j == 3)
        def _():
            for i in range(2, 4):
                for p in PEERS:
                    e1_fwd(i, p).start()

        pre_e(t)
        pre_h(t)

    def wgrad(l, hTl, eTl, b):
        for o in range(0, F, FW):
            acc1[l, :, o:o + FW] += nn(hTl, qb[b, :, o:o + FW])
            acc2[l, :, o:o + FW] += nn(eTl, gb[b, :, o:o + FW])

    def bx_step(t):
        jp = bx_jp(t)
        pr = PER * q + jp
        eb[0] = es[jp]

        def layer(li, carry):
            l = TOP - li
            b = li % PER

            @pl.when(li == 1)
            def _():
                f_drain_all()
                start_all(b_ins(0, pr, 0))

            @pl.when(li == TOP)
            def _():
                wait_all(b_ins(0, pr, 0))
                for i in range(2):
                    sv[i] = eb[0, i * CH:(i + 1) * CH, :]

            e = eb[0]
            eT = nt(sel[...], e).astype(bf16)
            va[...] = e.astype(f32)

            def up(o):
                p = nt(e, wb[l, o:o + FB, :]).astype(bf16).astype(f32)
                qv = (p * sb[b, :, o:o + FB]).astype(bf16)
                qb[b, :, o:o + FB] = qv
                return qv

            eb[0] = two_matmuls(va, up, lambda o, qv: nt(qv, wa[l, :, o:o + FB])).astype(bf16)

            @pl.when(li == TOP)
            def _():
                @pl.when(jp == 1)
                def _():
                    for i in range(2):
                        e_out(i).wait_send()

                eout[...] = eb[0]
                for i in range(2):
                    e_out(PER * jp + i).start()
                for i in range(2):
                    e1_save(PER * jp + i, i).start()

            wgrad(l, hT[l, pr], eT, b)

            @pl.when(jp == 1)
            def _():
                start_all(w_reload(l))

            return carry

        each_layer(layer)
        for i in range(2):
            e1_save(PER * jp + i, i).wait()

        @pl.when(jp == 1)
        def _():
            for p in PEERS:
                l_peer(p).start()
            for pair in (0, 2):
                for fwd in (e_fwd, e1_fwd):
                    for i in (pair, pair + 1):
                        for p in PEERS:
                            fwd(i, p).start()
            pre_h(t)

    def w_step(t):
        jp = w_jp(t)
        q_drain(t, 0)

        @pl.when(is_f_oth(t - 1))
        def _():
            wait_all(f_outs(2, 0, flip(t)))

        start_load(t, 1, flip(t))

        def layer(li, carry):
            l = TOP - li
            b = (t + li) % PER
            wait_all(w_ins(l, jp, b))

            @pl.when(li == 1)
            def _():
                pre_h(t)
                pre_e(t)

            wgrad(l, hT[l, PER * q + jp], eTs[jp, l], b)

            @pl.when(li == 0)
            def _():
                start_load(t, 2, b)

            @pl.when(li == 1)
            def _():
                start_load(t + 1, 0, b)

            return carry

        each_layer(layer)

    half_own = pl.ds(pl.multiple_of(96 * c, 8), 96)
    half_oth = pl.ds(pl.multiple_of(96 * (1 - c), 8), 96)

    def final_copies(l):
        lg = NL * c + l
        return [
            rcopy(acc1.at[l, half_oth, :], out_up.at[lg], xo_s.at[l, 0], xo_r.at[l, 0], partner),
            rcopy(acc2.at[l, half_oth, :], out_down.at[lg], xo_s.at[l, 1], xo_r.at[l, 1], partner),
            lcopy(acc1.at[l, half_own, :], out_up.at[lg], lo_s.at[l, 0]),
            lcopy(acc2.at[l, half_own, :], out_down.at[lg], lo_s.at[l, 1]),
        ]

    def b_oth(t):
        pr = b_pair(t)
        ei = t % PER
        first_load(t)

        @pl.when(first & ((t == 11) | (t == 13)))
        def _():
            for i in range(2):
                j = t - 11 + i
                wait_chunk(es, erecv, own0 + j)
                for p in PEERS:
                    e_fwd(j, p).start()

        @pl.when(is_ob(t))
        def _():
            eb[ei] = es[ob_jp(t)]

        @pl.when(jnp.logical_not(is_ob(t)))
        def _():
            e_in(pr, ei).wait()

        def layer(li, carry):
            l = TOP - li
            b = (t + li) % PER
            wait_all(b_ins(l, pr, b))
            q_drain(t, li)
            next_load(t, li, b)

            if not isinstance(li, int):
                @pl.when(li == jnp.where(is_ob(t), 2, 1))
                def _():
                    pre_e(t)

                @pl.when((li == 1) & jnp.logical_not(first))
                def _():
                    wait_pair(e1recv, pr)
                    e1_in(pr, ei).start()

                @pl.when((li == TOP) & jnp.logical_not(first))
                def _():
                    e1_in(pr, ei).wait()
                    eb[ei] = tgt[ei]

            e = eb[ei]
            eT = nt(sel[...], e).astype(bf16)
            for o in range(0, F, FW):
                p = nn(e, wa[l, :, o:o + FW]).astype(bf16).astype(f32)
                qb[b, :, o:o + FW] = (p * sb[b, :, o:o + FW]).astype(bf16)
            if isinstance(li, int):
                for o in range(0, D, DW):
                    eb[ei, :, o:o + DW] = (e[:, o:o + DW].astype(f32) + nn(qb[b], wb[l, :, o:o + DW])).astype(bf16)
            wgrad(l, hT[l, pr], eT, b)

            if not isinstance(li, int):
                @pl.when((li == 1) & first)
                def _():
                    for o in range(0, D, DW):
                        eb[ei, :, o:o + DW] = (eb[ei, :, o:o + DW].astype(f32) + nn(qb[b], wb[l, :, o:o + DW])).astype(bf16)

            @pl.when(t == end)
            def _():
                start_all(final_copies(l))

            return carry

        each_layer(layer, peel=True)

        @pl.when(last & (t == 13))
        def _():
            for p in PEERS:
                qo = (q + 1 + p) % 4
                rcopy(lmine, lbuf.at[qo], lsend.at[p], lrecv.at[qo], peers[p]).wait_recv()
            lbuf[q] = lmine[...]
            tot = (lbuf[0] + lbuf[1]) + (lbuf[2] + lbuf[3])
            loss_out[...] = jnp.zeros((8, 128), f32) + jnp.sum(tot) * (0.5 * inv_total)
            for kk in range(7):
                l_out(kk).start()

    def step(t, carry):
        for test, run in ((is_tr, tr_step), (is_f_own, f_own), (is_f_oth, f_oth), (is_b_own, b_own), (is_bx, bx_step), (is_w, w_step), (is_b_oth, b_oth)):
            @pl.when(test(t))
            def _():
                run(t)

        return carry

    lax.fori_loop(0, NSTEP, step, 0)

    for j in range(4):
        for p in PEERS:
            h_fwd(j, p).wait_send()
            e_fwd(j, p).wait_send()
            h2_fwd(j, p).wait_send()

    @pl.when(k > 0)
    def _():
        for j in range(4):
            for p in PEERS:
                e1_fwd(j, p).wait_send()

    @pl.when(k > 0)
    def _():
        for j in range(2, 4):
            e_out(j).wait_send()

    @pl.when(k < 7)
    def _():
        l_out(0).wait_recv()

    @pl.when(k == 1)
    def _():
        xcopy(0).wait_send()
        xcopy(1).wait_send()

    @pl.when(k == 6)
    def _():
        tcopy().wait_send()

    @pl.when(k == 7)
    def _():
        for p in PEERS:
            l_peer(p).wait_send()
        for kk in range(7):
            l_out(kk).wait_send()

    for l in range(NL):
        lg = NL * (1 - c) + l
        rcopy(acc1.at[l, half_oth, :], out_up.at[lg], xo_s.at[l, 0], xo_r.at[l, 0], partner).wait_recv()
        rcopy(acc2.at[l, half_oth, :], out_down.at[lg], xo_s.at[l, 1], xo_r.at[l, 1], partner).wait_recv()
        r1, r2, l1, l2 = final_copies(l)
        r1.wait_send()
        r2.wait_send()
        l1.wait()
        l2.wait()


def solution(mesh):
    n_data = mesh.shape["data"]

    def per_device(inputs, targets, w_up, w_down):
        n_micro, n_tok, width = inputs.shape
        inv_total = 1.0 / (n_data * n_micro * n_tok)
        x = inputs.reshape(n_micro * n_tok, width)
        y = targets.reshape(n_micro * n_tok, width)
        V = pltpu.VMEM
        DMA = pltpu.SemaphoreType.DMA
        S = jax.ShapeDtypeStruct
        anyspec = pl.BlockSpec(memory_space=pl.ANY)
        pairs = 8
        half_grad = S((PER * NL, D // pairs, F), f32)
        rows = S((pairs, PR, D), bf16)
        two_rows = V((PER, PR, D), bf16)
        two_wide = V((PER, PR, F), bf16)
        grads = V((NL, DS, F), f32)
        tile = V((8, 128), f32)
        two, four, by_layer, chunks, fan = DMA((PER,)), DMA((4,)), DMA((NL, PER)), DMA((16,)), DMA((4, 3))
        outs = pl.pallas_call(
            functools.partial(kernel, inv_total),
            out_shape=(
                S((8, 128), f32), half_grad, half_grad,
                S((NL, pairs, PR, F), f32), S((NL, pairs, PR, F), bf16), S((NL, PER, PR, F), bf16),
                S((NL, D, F), bf16), S((NL, F, D), bf16), rows, rows, rows, rows,
            ),
            in_specs=[anyspec] * 4,
            out_specs=(pl.BlockSpec(memory_space=pltpu.VMEM),) + (anyspec,) * 11,
            scratch_shapes=[
                V((NL, D, F), bf16), V((NL, F, D), bf16), grads, grads, two_rows, two_rows,
                V((PER, PR, F), f32), two_wide, two_wide,
                V((NL, pairs, DS, PR), bf16), V((PER, NL, DS, PR), bf16),
                two_rows, two_rows, V((PR, D), bf16), two_rows, V((PER, CH, D), bf16), V((PR, D), f32),
                V((DS, D), bf16), tile, V((4, 8, 128), f32), tile,
                by_layer, by_layer, chunks, chunks, fan, fan, two, two, chunks, chunks, two, four, two,
                fan, fan, four, four, DMA((1,)), DMA((3,)), DMA((7,)), DMA,
            ] + [two] * 9 + [DMA((6,)), by_layer, by_layer, by_layer],
            compiler_params=pltpu.CompilerParams(collective_id=0, has_side_effects=True, vmem_limit_bytes=67043328),
            name="stack_step",
        )(x, y, w_up, w_down)
        return outs[0][0, 0], outs[1], jnp.swapaxes(outs[2], 1, 2)

    return jax.shard_map(
        per_device,
        mesh=mesh,
        in_specs=(P("data", None, None), P("data", None, None), P("stage", None, None), P("stage", None, None)),
        out_specs=(P(), P("stage", "data", None), P("stage", None, "data")),
        check_vma=False,
    )
```

```python
import functools

import jax
import jax.numpy as jnp
from jax import lax
from jax.experimental import pallas as pl
from jax.experimental.pallas import tpu as pltpu
from jax.sharding import PartitionSpec as P

bf16, f32 = jnp.bfloat16, jnp.float32
MESH = pl.DeviceIdType.MESH
NT = (((1,), (1,)), ((), ()))
C0 = 0.7978845608028654
C1 = C0 * 0.044715
D, F = 768, 3072
CH, PR = 128, 256
NL = 3
DS = 192
FB, FW, DW = 512, 768, 256
BLOCKS = [i * FB for i in range(F // FB)]
NSTEP = 23
PER = 2
TOP = NL - 1
PEERS = range(3)
HEAD = slice(0, CH)


def each_layer(layer, peel=False):
    if peel:
        layer(0, 0)
    lax.fori_loop(int(peel), NL, layer, 0)


def flip(t):
    return (t + 1) % PER


def nn(a, b):
    return jnp.dot(a, b, preferred_element_type=f32)


def nt(a, b):
    return lax.dot_general(a, b, NT, preferred_element_type=f32)


def gelu_and_slope(u):
    s = u * u
    b = 0.5 + 0.5 * jnp.tanh(u * (C0 + C1 * s))
    g = u * b
    return g, b + (g * (1.0 - b)) * (2.0 * C0 + (6.0 * C1) * s)


def two_matmuls(va, first, second):
    v = first(BLOCKS[0])
    for o in BLOCKS[1:]:
        w = first(o)
        va[...] += second(o - FB, v)
        v = w
    return va[...] + second(BLOCKS[-1], v)


def kernel(inv_total, x_in, y_in, w_up, w_down,
           loss_out, out_up, out_down, s_hbm, g_hbm, q_hbm, wta, wtb, hx, ex, hx2, ex1,
           wa, wb, acc1, acc2, hs, es, sb, gb, qb, hT, eTs, hb, eb, eout, tgt, sv, va, sel, ltile, lbuf, lmine,
           wsem, rsem, h2recv, e1recv, h2fwd, e1fwd, is_x, os_x, hrecv, erecv, trecv, lrecv, xsend, hfwd, efwd, hsend, esend, tsend, lsend, lout_s, lout_r,
           os_s, os_g, os_q, is_s, is_g, is_q, is_h, is_e, tr_q, tr_h, xo_s, xo_r, lo_s):
    s = lax.axis_index("stage")
    d = lax.axis_index("data")
    c = d % PER
    q = d // PER
    k = PER * s + c
    nxt = (s + c, d + 1 - PER * c)
    prv = (s - 1 + c, d + 1 - PER * c)
    partner = (s, d + 1 - PER * c)
    peers = [(s, ((q + p) % 4) * 2 + c) for p in (1, 2, 3)]

    def rcopy(src, dst, ss, rs, dev):
        return pltpu.make_async_remote_copy(src_ref=src, dst_ref=dst, send_sem=ss, recv_sem=rs, device_id=dev, device_id_type=MESH)

    lcopy = pltpu.make_async_copy
    hc = hb.at[0, HEAD, :]
    ec = eb.at[0, HEAD, :]

    bar = pltpu.get_barrier_semaphore()
    for dev in peers:
        pl.semaphore_signal(bar, inc=1, device_id=dev, device_id_type=MESH)

    @pl.when(k < 7)
    def _():
        pl.semaphore_signal(bar, inc=1, device_id=nxt, device_id_type=MESH)

    @pl.when(k > 0)
    def _():
        pl.semaphore_signal(bar, inc=1, device_id=prv, device_id_type=MESH)

    @pl.when(k < 6)
    def _():
        pl.semaphore_signal(bar, inc=1, device_id=(3, PER * q + 1), device_id_type=MESH)

    def w_load(l):
        return (lcopy(w_up.at[NL * c + l], wa.at[l], wsem.at[l, 0]),
                lcopy(w_down.at[NL * c + l], wb.at[l], wsem.at[l, 1]))

    def w_reload(l):
        return (lcopy(wta.at[l], wa.at[l], rsem.at[l, 0]),
                lcopy(wtb.at[l], wb.at[l], rsem.at[l, 1]))

    def start_all(cps):
        for cp in cps:
            cp.start()

    def wait_all(cps):
        for cp in cps:
            cp.wait()

    def half(ch):
        return pl.ds(pl.multiple_of((ch % PER) * CH, CH), CH)

    def own(ref, j):
        return ref.at[j // PER, half(j), :]

    own0 = 4 * q

    @pl.when(k == 0)
    def _():
        for j in range(2):
            lcopy(x_in.at[pl.ds(j * CH, CH), :], own(hs, j), hrecv.at[own0 + j]).start()

    for l in range(NL):
        start_all(w_load(l))

    @pl.when(k == 7)
    def _():
        lcopy(y_in, tgt.at[1], trecv.at[1]).start()

    row = lax.broadcasted_iota(jnp.int32, (DS, D), 0)
    col = lax.broadcasted_iota(jnp.int32, (DS, D), 1)
    sel[...] = jnp.where(col == row + DS * q, 1.0, 0.0).astype(bf16)
    ltile[...] = jnp.zeros_like(ltile)

    pl.semaphore_wait(bar, 3 + jnp.where(k < 7, 1, 7) + jnp.where((k > 0) & (k < 7), 1, 0))

    def xcopy(j):
        return rcopy(x_in.at[pl.ds(j * CH, CH), :], own(hs, 2 + j), xsend.at[j], hrecv.at[own0 + 2 + j], partner)

    def tcopy():
        return rcopy(y_in, tgt.at[0], tsend.at[0], trecv.at[0], partner)

    @pl.when(k == 1)
    def _():
        xcopy(0).start()
        xcopy(1).start()

    @pl.when(k == 6)
    def _():
        tcopy().start()

    def h_fwd(j, p):
        ch = own0 + j
        return rcopy(own(hs, j), hx.at[ch // PER, half(ch), :], hfwd.at[j, p], hrecv.at[ch], peers[p])

    def e_fwd(j, p):
        ch = own0 + j
        return rcopy(own(es, j), ex.at[ch // PER, half(ch), :], efwd.at[j, p], erecv.at[ch], peers[p])

    def h2_fwd(j, p):
        ch = own0 + j
        at = hx2.at[ch // PER, half(ch), :]
        return rcopy(at, at, h2fwd.at[j, p], h2recv.at[ch], peers[p])

    def e1_fwd(j, p):
        ch = own0 + j
        at = ex1.at[ch // PER, half(ch), :]
        return rcopy(at, at, e1fwd.at[j, p], e1recv.at[ch], peers[p])

    def h2_save(j):
        ch = own0 + j
        return lcopy(sv.at[1], hx2.at[ch // PER, half(ch), :], os_x.at[0])

    def e1_save(j, b):
        ch = own0 + j
        return lcopy(sv.at[b], ex1.at[ch // PER, half(ch), :], os_x.at[b])

    def h_out(j):
        return rcopy(own(tgt, j), own(hs, j), hsend.at[j], hrecv.at[own0 + j], nxt)

    def e_out(j):
        return rcopy(eout.at[half(j), :], own(es, j), esend.at[j], erecv.at[own0 + j], prv)

    def l_peer(p):
        return rcopy(lmine, lbuf.at[q], lsend.at[p], lrecv.at[q], peers[p])

    def l_out(kk):
        return rcopy(loss_out, loss_out, lout_s.at[kk], lout_r, (kk // PER, PER * q + kk % PER))

    def wait_chunk(buf, sems, ch):
        rcopy(own(buf, 0), own(buf, 0), hfwd.at[0, 0], sems.at[ch], peers[0]).wait_recv()

    def s_out_own(l, ch, b):
        return lcopy(sb.at[b, half(ch), :], s_hbm.at[l, ch // PER, half(ch), :], os_s.at[b])

    def g_out_own(l, ch, b):
        return lcopy(gb.at[b, half(ch), :], g_hbm.at[l, ch // PER, half(ch), :], os_g.at[b])

    def q_out_own(l, j, b):
        return lcopy(qb.at[b, HEAD, :], q_hbm.at[l, j // PER, half(j), :], os_q.at[b])

    def f_drain(b):
        s_out_own(0, 0, b).wait()
        g_out_own(0, 0, b).wait()

    def f_drain_all():
        for b in range(PER):
            f_drain(b)

    def f_outs(l, pr, b):
        return lcopy(sb.at[b], s_hbm.at[l, pr], os_s.at[b]), lcopy(gb.at[b], g_hbm.at[l, pr], os_g.at[b])

    def s_in_own(l, ch, b):
        return lcopy(s_hbm.at[l, ch // PER, half(ch), :], sb.at[b, HEAD, :], is_s.at[b])

    def b_ins(l, pr, b):
        return lcopy(s_hbm.at[l, pr], sb.at[b], is_s.at[b]), lcopy(g_hbm.at[l, pr], gb.at[b], is_g.at[b])

    def w_ins(l, jp, b):
        return lcopy(q_hbm.at[l, jp], qb.at[b], is_q.at[b]), lcopy(g_hbm.at[l, PER * q + jp], gb.at[b], is_g.at[b])

    def h_in(pr, b):
        return lcopy(hx.at[pr], hb.at[b], is_h.at[b])

    def e_in(pr, b):
        return lcopy(ex.at[pr], eb.at[b], is_e.at[b])

    def h2_in(pr, b):
        return lcopy(hx2.at[pr], tgt.at[b], is_x.at[b])

    def e1_in(pr, b):
        return lcopy(ex1.at[pr], tgt.at[b], is_x.at[b])

    def wait_pair(sems, pr):
        wait_chunk(hs, sems, PER * pr)
        wait_chunk(hs, sems, PER * pr + 1)

    def ob_save(b):
        return lcopy(eb.at[b], ex1.at[PER * q + 1], os_x.at[b])

    first, last = k == 0, k == 7
    mid = (k > 0) & (k < 7)
    high = k >= 4

    def flag(x):
        return jnp.where(x, 1, 0)

    m = 6 * flag(k < 3) + 4 * flag(k == 3) + 3 * flag(k == 4) + 2 * flag(k == 5)
    end = jnp.where(mid, 22, 18)

    def within(t, a, b):
        return (t >= a) & (t < b)

    def is_tr(t):
        return t == jnp.where(high, 0, 4)

    def is_bx(t):
        return last & ((t == 3) | (t == 6))

    def bx_jp(t):
        return t // 6

    def is_f_own(t):
        return within(t, 0, jnp.where(last, 6, 5)) & jnp.logical_not(is_tr(t) | is_bx(t))

    def f_own_j(t):
        return jnp.where(high, t - 1, t) - flag(last & (t > 3))

    def is_b_own(t):
        return mid & (within(t, 5 + m, 7 + m) | within(t, 8 + m, 10 + m))

    def b_own_j(t):
        return t - 5 - m - flag(t > 7 + m)

    def is_w(t):
        return mid & (within(t, jnp.where(high, 15, 10 + m), jnp.where(high, 17, 11 + m)) | (is_gap(t) & jnp.logical_not(high)))

    def w_jp(t):
        return jnp.where(high, t - 15, flag(t > 7 + m))

    def is_ob(t):
        return first & ((t == 11) | (t == 14))

    def ob_jp(t):
        return t // 14

    def is_gap(t):
        return mid & (t == 7 + m)

    def is_b_oth(t):
        return (mid & within(t, 17, 23)) | (first & within(t, 11, 19)) | (last & within(t, 13, 19))

    def is_f_oth(t):
        return (first & within(t, 5, 11)) | (last & within(t, 7, 13)) | (is_gap(t) & high) | (mid & (within(t, 5, 5 + m) | within(t, jnp.where(high, 10, 11) + m, jnp.where(high, 15, 17))))

    def oth_pair(i):
        return 2 * ((q + 1 + i % 3) % 4) + i // 3

    def f_pair(t):
        i = jnp.where(t < 5 + m, t - 5, jnp.where(is_gap(t), m, jnp.where(high, t - 9, t - 11)))
        return oth_pair(jnp.where(last, t - 7, i))

    def b_pair(t):
        i0 = jnp.where(t < 14, t - 12, t - 13)
        i = jnp.where(first, i0, jnp.where(last, t - 13, t - 17))
        return jnp.where(is_ob(t), PER * q + ob_jp(t), oth_pair(jnp.maximum(i, 0)))

    def is_loader(t):
        return is_b_own(t) | is_w(t) | is_b_oth(t)

    def start_load(t, li, b):
        l = TOP - li

        @pl.when(is_b_own(t))
        def _():
            s_in_own(l, own0 + b_own_j(t), b).start()

        @pl.when(is_w(t))
        def _():
            start_all(w_ins(l, w_jp(t), b))

        @pl.when(is_b_oth(t))
        def _():
            start_all(b_ins(l, b_pair(t), b))

    def next_load(t, li, b):
        @pl.when(li < 2)
        def _():
            start_load(t, li + 1, 1 - b)

        @pl.when(li == TOP)
        def _():
            start_load(t + 1, 0, 1 - b)

    def first_load(t):
        @pl.when(is_f_oth(t - 1))
        def _():
            wait_all(f_outs(2, 0, flip(t)))

        @pl.when(is_f_own(t - 1))
        def _():
            f_drain_all()

        @pl.when(jnp.logical_not(is_loader(t - 1) | is_f_oth(t - 1) | is_f_own(t - 1)))
        def _():
            start_load(t, 0, t % PER)

    def pre_h(t):
        @pl.when(is_f_oth(t + 1))
        def _():
            pr = f_pair(t + 1)
            wait_chunk(hs, hrecv, PER * pr)
            wait_chunk(hs, hrecv, PER * pr + 1)
            h_in(pr, flip(t)).start()

    def pre_e(t):
        @pl.when(is_b_oth(t + 1) & jnp.logical_not(is_ob(t + 1)))
        def _():
            pr = b_pair(t + 1)
            wait_chunk(es, erecv, PER * pr)
            wait_chunk(es, erecv, PER * pr + 1)
            e_in(pr, flip(t)).start()

    def wait_reload(t, l):
        @pl.when(t == jnp.where(last, 7, 5))
        def _():
            wait_all(w_reload(l))

    def tr_step(t):
        def zero(i, carry):
            r = pl.ds(pl.multiple_of(i * 8, 8), 8)
            for l in range(NL):
                acc1[l, r, :] = jnp.zeros((8, F), f32)
                acc2[l, r, :] = jnp.zeros((8, F), f32)
            return carry

        lax.fori_loop(0, DS // 8, zero, 0)

        @pl.when(jnp.logical_not(high))
        def _():
            f_drain_all()

        stage = [hb.at[0], hb.at[1], eb.at[0], eb.at[1], eout]
        pend_q, pend_h = [None] * 2, [None] * 5

        def reload(l):
            @pl.when(jnp.logical_not(high))
            def _():
                start_all(w_reload(l))

        def put(pend, sems, n, buf, src, dst):
            if pend[n] is not None:
                pend[n].wait()
            for o in range(0, src.shape[0], D):
                buf[:, o:o + D] = src[o:o + D, :].T
            pend[n] = lcopy(buf, dst, sems.at[n])
            pend[n].start()

        for l in range(NL):
            @pl.when(high)
            def _():
                wait_all(w_load(l))

            for i in range(3):
                put(pend_q, tr_q, i % PER, qb.at[i % PER], wb.at[l, :, pl.ds(i * 256, 256)], wta.at[l, pl.ds(i * 256, 256), :])
                for r in range(4 * i, 4 * i + 4):
                    put(pend_h, tr_h, r % 5, stage[r % 5], wa.at[l, :, pl.ds(r * 256, 256)], wtb.at[l, pl.ds(r * 256, 256), :])
            if l > 0:
                reload(l - 1)
        wait_all(pend_q + pend_h)
        reload(NL - 1)
        pre_h(t)

    def f_own(t):
        j = f_own_j(t)
        ch = own0 + j
        rows = half(j)
        wait_chunk(hs, hrecv, ch)
        for p in PEERS:
            h_fwd(j, p).start()
        hc[...] = hs[j // PER, rows, :]

        def layer(l, carry):
            b = l % PER

            @pl.when((j == 0) & jnp.logical_not(high))
            def _():
                wait_all(w_load(l))

            @pl.when((l == TOP) | is_f_own(t - 1))
            def _():
                f_drain(b)

            @pl.when((k == 6) & (j == 3) & (l == 1))
            def _():
                for i in range(PER):
                    start_load(t + 1, i, 1 - i)

            h = hc[...]

            sv[jnp.maximum(l - 1, 0)] = h
            acc = va.at[HEAD, :]
            acc[...] = h.astype(f32)

            def up(o):
                g, slope = gelu_and_slope(nn(h, wa[l, :, o:o + FB]))
                sb[b, rows, o:o + FB] = slope
                g = g.astype(bf16)
                gb[b, rows, o:o + FB] = g
                return g

            hc[...] = two_matmuls(acc, up, lambda o, g: nn(g, wb[l, o:o + FB, :])).astype(bf16)
            s_out_own(l, ch, b).start()
            g_out_own(l, ch, b).start()

            @pl.when((j == 3) & within(k, 4, 6))
            def _():
                start_all(w_reload(l))

            @pl.when((j == 3) & (k == 6) & (l == TOP))
            def _():
                for i in reversed(range(NL)):
                    start_all(w_reload(i))

            return carry

        each_layer(layer)

        @pl.when(k < 7)
        def _():
            tgt[j // PER, rows, :] = hc[...]
            h_out(j).start()

        @pl.when(k == 7)
        def _():
            @pl.when(j == 0)
            def _():
                rcopy(y_in, tgt.at[0], tsend.at[0], trecv.at[0], partner).wait_recv()

            @pl.when(j == 2)
            def _():
                lcopy(y_in, tgt.at[1], trecv.at[1]).wait()

            diff = hc[...].astype(f32) - tgt[j // PER, rows, :].astype(f32)
            es[j // PER, rows, :] = (diff * inv_total).astype(bf16)
            sq = jnp.sum((diff * diff).reshape(CH // 8, 8, D), axis=0)
            ltile[...] += sum(sq[:, i * 128:(i + 1) * 128] for i in range(D // 128))

            @pl.when(j == 3)
            def _():
                lmine[...] = ltile[...]

        h2_save(j).start()
        hT[0, ch // PER, :, rows] = nt(sel[...], hs[j // PER, rows, :]).astype(bf16)
        for l in range(1, NL):
            hT[l, ch // PER, :, rows] = nt(sel[...], sv[l - 1]).astype(bf16)
        h2_save(j).wait()
        for p in PEERS:
            h2_fwd(j, p).start()
        pre_h(t)

    def q_drain(t, li):
        @pl.when((li == flag(is_b_own(t))) & is_b_own(t - 1))
        def _():
            q_out_own(0, 0, flip(t)).wait()

    def f_oth(t):
        pr = f_pair(t)
        hi = t % PER

        @pl.when(is_f_own(t - 1))
        def _():
            f_drain_all()

        q_drain(t, 0)

        @pl.when((k < 7) & (t == 5 + 2 * flag(k == 6)))
        def _():
            for j in range(4):
                h_out(j).wait_send()

        h_in(pr, hi).wait()

        def layer(l, carry):
            b = (t + l) % PER
            wait_reload(t, l)

            if not isinstance(l, int):
                @pl.when((l == 1) & is_f_oth(t - 1))
                def _():
                    wait_all(f_outs(2, 0, b))

                @pl.when(l == 1)
                def _():
                    wait_pair(h2recv, pr)
                    h2_in(pr, hi).start()
                    pre_h(t)
                    pre_e(t)

                @pl.when(l == TOP)
                def _():
                    wait_all(f_outs(0, pr, b))
                    h2_in(pr, hi).wait()
                    hb[hi] = tgt[hi]

            h = hb[hi]
            hT[l, pr] = nt(sel[...], h).astype(bf16)

            def up(o):
                g, slope = gelu_and_slope(nt(h, wb[l, o:o + FB, :]))
                sb[b, :, o:o + FB] = slope
                g = g.astype(bf16)
                gb[b, :, o:o + FB] = g
                return g

            if isinstance(l, int):
                va[...] = h.astype(f32)
                hb[hi] = two_matmuls(va, up, lambda o, g: nt(g, wa[l, :, o:o + FB])).astype(bf16)
            else:
                for o in BLOCKS:
                    up(o)
            start_all(f_outs(l, pr, b))
            return carry

        each_layer(layer, peel=True)
        wait_all(f_outs(1, pr, flip(t)))

        @pl.when(is_loader(t + 1))
        def _():
            start_load(t + 1, 0, flip(t))

    def b_own(t):
        j = b_own_j(t)
        ch = own0 + j
        jp = j // PER
        first_load(t)
        wait_chunk(es, erecv, ch)
        for p in PEERS:
            e_fwd(j, p).start()
        ec[...] = es[jp, half(j), :]

        def layer(li, carry):
            l = TOP - li
            b = (t + li) % PER
            s_in_own(l, ch, b).wait()
            q_drain(t, li)

            @pl.when(li == TOP)
            def _():
                q_out_own(2, j, b).wait()
                q_out_own(1, j, 1 - b).wait()


            @pl.when((li > 0) | jnp.logical_not(is_f_own(t - 1)))
            def _():
                next_load(t, li, b)

            wait_reload(t, l)
            e = ec[...]

            sv[jnp.maximum(li - 1, 0)] = e
            acc = va.at[HEAD, :]
            acc[...] = e.astype(f32)

            def up(o):
                p = nn(e, wa[l, :, o:o + FB]).astype(bf16).astype(f32)
                qv = (p * sb[b, HEAD, o:o + FB]).astype(bf16)
                qb[b, HEAD, o:o + FB] = qv
                return qv

            ec[...] = two_matmuls(acc, up, lambda o, qv: nn(qv, wb[l, o:o + FB, :])).astype(bf16)
            q_out_own(l, j, b).start()
            return carry

        each_layer(layer)
        @pl.when(j >= 2)
        def _():
            e_out(j - 2).wait_send()

        eout[half(j), :] = ec[...]
        e_out(j).start()
        e1_save(j, 1).start()
        eTs[jp, 2, :, half(j)] = nt(sel[...], es[jp, half(j), :]).astype(bf16)
        for li in range(1, NL):
            eTs[jp, TOP - li, :, half(j)] = nt(sel[...], sv[li - 1]).astype(bf16)
        e1_save(j, 1).wait()

        @pl.when(j == jnp.where(k > 1, 1, 2))
        def _():
            for i in range(2):
                for p in PEERS:
                    e1_fwd(i, p).start()

        @pl.when(j == 3)
        def _():
            for i in range(2, 4):
                for p in PEERS:
                    e1_fwd(i, p).start()

        pre_e(t)
        pre_h(t)

    def wgrad(l, hTl, eTl, b):
        for o in range(0, F, FW):
            acc1[l, :, o:o + FW] += nn(hTl, qb[b, :, o:o + FW])
            acc2[l, :, o:o + FW] += nn(eTl, gb[b, :, o:o + FW])

    def bx_step(t):
        jp = bx_jp(t)
        pr = PER * q + jp
        eb[0] = es[jp]

        def layer(li, carry):
            l = TOP - li
            b = li % PER

            @pl.when(li == 1)
            def _():
                f_drain_all()
                start_all(b_ins(0, pr, 0))

            @pl.when(li == TOP)
            def _():
                wait_all(b_ins(0, pr, 0))
                for i in range(2):
                    sv[i] = eb[0, i * CH:(i + 1) * CH, :]

            e = eb[0]
            eT = nt(sel[...], e).astype(bf16)
            va[...] = e.astype(f32)

            def up(o):
                p = nt(e, wb[l, o:o + FB, :]).astype(bf16).astype(f32)
                qv = (p * sb[b, :, o:o + FB]).astype(bf16)
                qb[b, :, o:o + FB] = qv
                return qv

            eb[0] = two_matmuls(va, up, lambda o, qv: nt(qv, wa[l, :, o:o + FB])).astype(bf16)

            @pl.when(li == TOP)
            def _():
                @pl.when(jp == 1)
                def _():
                    for i in range(2):
                        e_out(i).wait_send()

                eout[...] = eb[0]
                for i in range(2):
                    e_out(PER * jp + i).start()
                for i in range(2):
                    e1_save(PER * jp + i, i).start()

            wgrad(l, hT[l, pr], eT, b)

            @pl.when(jp == 1)
            def _():
                start_all(w_reload(l))

            return carry

        each_layer(layer)
        for i in range(2):
            e1_save(PER * jp + i, i).wait()

        @pl.when(jp == 1)
        def _():
            for p in PEERS:
                l_peer(p).start()
            for pair in (0, 2):
                for fwd in (e_fwd, e1_fwd):
                    for i in (pair, pair + 1):
                        for p in PEERS:
                            fwd(i, p).start()
            pre_h(t)

    def w_step(t):
        jp = w_jp(t)
        q_drain(t, 0)

        @pl.when(is_f_oth(t - 1))
        def _():
            wait_all(f_outs(2, 0, flip(t)))

        start_load(t, 1, flip(t))

        def layer(li, carry):
            l = TOP - li
            b = (t + li) % PER
            wait_all(w_ins(l, jp, b))

            @pl.when(li == 1)
            def _():
                pre_h(t)
                pre_e(t)

            wgrad(l, hT[l, PER * q + jp], eTs[jp, l], b)

            @pl.when(li == 0)
            def _():
                start_load(t, 2, b)

            @pl.when(li == 1)
            def _():
                start_load(t + 1, 0, b)

            return carry

        each_layer(layer)

    half_own = pl.ds(pl.multiple_of(96 * c, 8), 96)
    half_oth = pl.ds(pl.multiple_of(96 * (1 - c), 8), 96)

    def final_copies(l):
        lg = NL * c + l
        return [
            rcopy(acc1.at[l, half_oth, :], out_up.at[lg], xo_s.at[l, 0], xo_r.at[l, 0], partner),
            rcopy(acc2.at[l, half_oth, :], out_down.at[lg], xo_s.at[l, 1], xo_r.at[l, 1], partner),
            lcopy(acc1.at[l, half_own, :], out_up.at[lg], lo_s.at[l, 0]),
            lcopy(acc2.at[l, half_own, :], out_down.at[lg], lo_s.at[l, 1]),
        ]

    def b_oth(t):
        pr = b_pair(t)
        ei = t % PER
        inner = jnp.logical_not(first) | (t > 16)
        first_load(t)

        for j, at in ((0, 11), (1, 11), (2, 13), (3, 14)):
            @pl.when(first & (t == at))
            def _():
                wait_chunk(es, erecv, own0 + j)
                for p in PEERS:
                    e_fwd(j, p).start()

        @pl.when(is_ob(t))
        def _():
            eb[ei] = es[ob_jp(t)]

        @pl.when(jnp.logical_not(is_ob(t)))
        def _():
            e_in(pr, ei).wait()

        def layer(li, carry):
            l = TOP - li
            b = (t + li) % PER
            wait_all(b_ins(l, pr, b))
            q_drain(t, li)
            next_load(t, li, b)

            if not isinstance(li, int):
                @pl.when(li == jnp.where(is_ob(t), 2, 1))
                def _():
                    pre_e(t)

                @pl.when((li == 1) & inner)
                def _():
                    wait_pair(e1recv, pr)
                    e1_in(pr, ei).start()

                @pl.when((li == TOP) & inner)
                def _():
                    e1_in(pr, ei).wait()
                    eb[ei] = tgt[ei]

                @pl.when((li == TOP) & first & (t == 14))
                def _():
                    ob_save(ei).start()

            e = eb[ei]
            eT = nt(sel[...], e).astype(bf16)
            for o in range(0, F, FW):
                p = nn(e, wa[l, :, o:o + FW]).astype(bf16).astype(f32)
                qb[b, :, o:o + FW] = (p * sb[b, :, o:o + FW]).astype(bf16)
            if isinstance(li, int):
                for o in range(0, D, DW):
                    eb[ei, :, o:o + DW] = (e[:, o:o + DW].astype(f32) + nn(qb[b], wb[l, :, o:o + DW])).astype(bf16)
            wgrad(l, hT[l, pr], eT, b)

            if not isinstance(li, int):
                @pl.when((li == 1) & jnp.logical_not(inner))
                def _():
                    for o in range(0, D, DW):
                        eb[ei, :, o:o + DW] = (eb[ei, :, o:o + DW].astype(f32) + nn(qb[b], wb[l, :, o:o + DW])).astype(bf16)

            @pl.when(t == end)
            def _():
                start_all(final_copies(l))

            return carry

        each_layer(layer, peel=True)

        @pl.when(first & (t == 14))
        def _():
            ob_save(ei).wait()
            for j in range(2, 4):
                for p in PEERS:
                    e1_fwd(j, p).start()

        @pl.when(last & (t == 13))
        def _():
            for p in PEERS:
                qo = (q + 1 + p) % 4
                rcopy(lmine, lbuf.at[qo], lsend.at[p], lrecv.at[qo], peers[p]).wait_recv()
            lbuf[q] = lmine[...]
            tot = (lbuf[0] + lbuf[1]) + (lbuf[2] + lbuf[3])
            loss_out[...] = jnp.zeros((8, 128), f32) + jnp.sum(tot) * (0.5 * inv_total)
            for kk in range(7):
                l_out(kk).start()

    def step(t, carry):
        for test, run in ((is_tr, tr_step), (is_f_own, f_own), (is_f_oth, f_oth), (is_b_own, b_own), (is_bx, bx_step), (is_w, w_step), (is_b_oth, b_oth)):
            @pl.when(test(t))
            def _():
                run(t)

        return carry

    lax.fori_loop(0, NSTEP, step, 0)

    @pl.when(first)
    def _():
        wait_pair(e1recv, oth_pair(3))

    for j in range(4):
        for p in PEERS:
            h_fwd(j, p).wait_send()
            e_fwd(j, p).wait_send()
            h2_fwd(j, p).wait_send()

    for j in range(4):
        @pl.when((k > 0) | (j > 1))
        def _():
            for p in PEERS:
                e1_fwd(j, p).wait_send()

    @pl.when(k > 0)
    def _():
        for j in range(2, 4):
            e_out(j).wait_send()

    @pl.when(k < 7)
    def _():
        l_out(0).wait_recv()

    @pl.when(k == 1)
    def _():
        xcopy(0).wait_send()
        xcopy(1).wait_send()

    @pl.when(k == 6)
    def _():
        tcopy().wait_send()

    @pl.when(k == 7)
    def _():
        for p in PEERS:
            l_peer(p).wait_send()
        for kk in range(7):
            l_out(kk).wait_send()

    for l in range(NL):
        lg = NL * (1 - c) + l
        rcopy(acc1.at[l, half_oth, :], out_up.at[lg], xo_s.at[l, 0], xo_r.at[l, 0], partner).wait_recv()
        rcopy(acc2.at[l, half_oth, :], out_down.at[lg], xo_s.at[l, 1], xo_r.at[l, 1], partner).wait_recv()
        r1, r2, l1, l2 = final_copies(l)
        r1.wait_send()
        r2.wait_send()
        l1.wait()
        l2.wait()


def solution(mesh):
    n_data = mesh.shape["data"]

    def per_device(inputs, targets, w_up, w_down):
        n_micro, n_tok, width = inputs.shape
        inv_total = 1.0 / (n_data * n_micro * n_tok)
        x = inputs.reshape(n_micro * n_tok, width)
        y = targets.reshape(n_micro * n_tok, width)
        V = pltpu.VMEM
        DMA = pltpu.SemaphoreType.DMA
        S = jax.ShapeDtypeStruct
        anyspec = pl.BlockSpec(memory_space=pl.ANY)
        pairs = 8
        half_grad = S((PER * NL, D // pairs, F), f32)
        rows = S((pairs, PR, D), bf16)
        two_rows = V((PER, PR, D), bf16)
        two_wide = V((PER, PR, F), bf16)
        grads = V((NL, DS, F), f32)
        tile = V((8, 128), f32)
        two, four, by_layer, chunks, fan = DMA((PER,)), DMA((4,)), DMA((NL, PER)), DMA((16,)), DMA((4, 3))
        outs = pl.pallas_call(
            functools.partial(kernel, inv_total),
            out_shape=(
                S((8, 128), f32), half_grad, half_grad,
                S((NL, pairs, PR, F), f32), S((NL, pairs, PR, F), bf16), S((NL, PER, PR, F), bf16),
                S((NL, D, F), bf16), S((NL, F, D), bf16), rows, rows, rows, rows,
            ),
            in_specs=[anyspec] * 4,
            out_specs=(pl.BlockSpec(memory_space=pltpu.VMEM),) + (anyspec,) * 11,
            scratch_shapes=[
                V((NL, D, F), bf16), V((NL, F, D), bf16), grads, grads, two_rows, two_rows,
                V((PER, PR, F), f32), two_wide, two_wide,
                V((NL, pairs, DS, PR), bf16), V((PER, NL, DS, PR), bf16),
                two_rows, two_rows, V((PR, D), bf16), two_rows, V((PER, CH, D), bf16), V((PR, D), f32),
                V((DS, D), bf16), tile, V((4, 8, 128), f32), tile,
                by_layer, by_layer, chunks, chunks, fan, fan, two, two, chunks, chunks, two, four, two,
                fan, fan, four, four, DMA((1,)), DMA((3,)), DMA((7,)), DMA,
            ] + [two] * 9 + [DMA((6,)), by_layer, by_layer, by_layer],
            compiler_params=pltpu.CompilerParams(collective_id=0, has_side_effects=True, vmem_limit_bytes=67043328),
            name="stack_step",
        )(x, y, w_up, w_down)
        return outs[0][0, 0], outs[1], jnp.swapaxes(outs[2], 1, 2)

    return jax.shard_map(
        per_device,
        mesh=mesh,
        in_specs=(P("data", None, None), P("data", None, None), P("stage", None, None), P("stage", None, None)),
        out_specs=(P(), P("stage", "data", None), P("stage", None, "data")),
        check_vma=False,
    )
```

```python
import functools

import jax
import jax.numpy as jnp
from jax import lax
from jax.experimental import pallas as pl
from jax.experimental.pallas import tpu as pltpu
from jax.sharding import PartitionSpec as P

bf16, f32 = jnp.bfloat16, jnp.float32
MESH = pl.DeviceIdType.MESH
NT = (((1,), (1,)), ((), ()))
C0 = 0.7978845608028654
C1 = C0 * 0.044715
D, F = 768, 3072
CH, PR = 128, 256
NL = 3
DS = 192
FB, FW, DW = 512, 768, 256
BLOCKS = [i * FB for i in range(F // FB)]
NSTEP = 23
PER = 2
TOP = NL - 1
PEERS = range(3)
HEAD = slice(0, CH)


def each_layer(layer, peel=False):
    if peel:
        layer(0, 0)
    lax.fori_loop(int(peel), NL, layer, 0)


def flip(t):
    return (t + 1) % PER


def nn(a, b):
    return jnp.dot(a, b, preferred_element_type=f32)


def nt(a, b):
    return lax.dot_general(a, b, NT, preferred_element_type=f32)


def gelu_and_slope(u):
    s = u * u
    b = 0.5 + 0.5 * jnp.tanh(u * (C0 + C1 * s))
    g = u * b
    return g, b + (g * (1.0 - b)) * (2.0 * C0 + (6.0 * C1) * s)


def two_matmuls(va, first, second):
    v = first(BLOCKS[0])
    for o in BLOCKS[1:]:
        w = first(o)
        va[...] += second(o - FB, v)
        v = w
    return va[...] + second(BLOCKS[-1], v)


def kernel(inv_total, x_in, y_in, w_up, w_down,
           loss_out, out_up, out_down, s_hbm, g_hbm, q_hbm, wta, wtb, hx, ex, hx2, ex1,
           wa, wb, acc1, acc2, hs, es, sb, gb, qb, hT, eTs, hb, eb, eout, tgt, sv, va, sel, ltile, lbuf, lmine,
           wsem, rsem, h2recv, e1recv, h2fwd, e1fwd, is_x, os_x, hrecv, erecv, trecv, lrecv, xsend, hfwd, efwd, hsend, esend, tsend, lsend, lout_s, lout_r,
           os_s, os_g, os_q, is_s, is_g, is_q, is_h, is_e, tr_q, tr_h, xo_s, xo_r, lo_s):
    s = lax.axis_index("stage")
    d = lax.axis_index("data")
    c = d % PER
    q = d // PER
    k = PER * s + c
    nxt = (s + c, d + 1 - PER * c)
    prv = (s - 1 + c, d + 1 - PER * c)
    partner = (s, d + 1 - PER * c)
    peers = [(s, ((q + p) % 4) * 2 + c) for p in (1, 2, 3)]

    def rcopy(src, dst, ss, rs, dev):
        return pltpu.make_async_remote_copy(src_ref=src, dst_ref=dst, send_sem=ss, recv_sem=rs, device_id=dev, device_id_type=MESH)

    lcopy = pltpu.make_async_copy
    hc = hb.at[0, HEAD, :]
    ec = eb.at[0, HEAD, :]

    bar = pltpu.get_barrier_semaphore()
    for dev in peers:
        pl.semaphore_signal(bar, inc=1, device_id=dev, device_id_type=MESH)

    @pl.when(k < 7)
    def _():
        pl.semaphore_signal(bar, inc=1, device_id=nxt, device_id_type=MESH)

    @pl.when(k > 0)
    def _():
        pl.semaphore_signal(bar, inc=1, device_id=prv, device_id_type=MESH)

    @pl.when(k < 6)
    def _():
        pl.semaphore_signal(bar, inc=1, device_id=(3, PER * q + 1), device_id_type=MESH)

    def w_load(l):
        return (lcopy(w_up.at[NL * c + l], wa.at[l], wsem.at[l, 0]),
                lcopy(w_down.at[NL * c + l], wb.at[l], wsem.at[l, 1]))

    def w_reload(l):
        return (lcopy(wta.at[l], wa.at[l], rsem.at[l, 0]),
                lcopy(wtb.at[l], wb.at[l], rsem.at[l, 1]))

    def start_all(cps):
        for cp in cps:
            cp.start()

    def wait_all(cps):
        for cp in cps:
            cp.wait()

    def half(ch):
        return pl.ds(pl.multiple_of((ch % PER) * CH, CH), CH)

    def own(ref, j):
        return ref.at[j // PER, half(j), :]

    own0 = 4 * q

    @pl.when(k == 0)
    def _():
        for j in range(2):
            lcopy(x_in.at[pl.ds(j * CH, CH), :], own(hs, j), hrecv.at[own0 + j]).start()

    for l in range(NL):
        start_all(w_load(l))

    @pl.when(k == 7)
    def _():
        lcopy(y_in, tgt.at[1], trecv.at[1]).start()

    row = lax.broadcasted_iota(jnp.int32, (DS, D), 0)
    col = lax.broadcasted_iota(jnp.int32, (DS, D), 1)
    sel[...] = jnp.where(col == row + DS * q, 1.0, 0.0).astype(bf16)
    ltile[...] = jnp.zeros_like(ltile)

    pl.semaphore_wait(bar, 3 + jnp.where(k < 7, 1, 7) + jnp.where((k > 0) & (k < 7), 1, 0))

    def xcopy(j):
        return rcopy(x_in.at[pl.ds(j * CH, CH), :], own(hs, 2 + j), xsend.at[j], hrecv.at[own0 + 2 + j], partner)

    def tcopy():
        return rcopy(y_in, tgt.at[0], tsend.at[0], trecv.at[0], partner)

    @pl.when(k == 1)
    def _():
        xcopy(0).start()
        xcopy(1).start()

    @pl.when(k == 6)
    def _():
        tcopy().start()

    def h_fwd(j, p):
        ch = own0 + j
        return rcopy(own(hs, j), hx.at[ch // PER, half(ch), :], hfwd.at[j, p], hrecv.at[ch], peers[p])

    def e_fwd(j, p):
        ch = own0 + j
        return rcopy(own(es, j), ex.at[ch // PER, half(ch), :], efwd.at[j, p], erecv.at[ch], peers[p])

    def h2_fwd(j, p):
        ch = own0 + j
        at = hx2.at[ch // PER, half(ch), :]
        return rcopy(at, at, h2fwd.at[j, p], h2recv.at[ch], peers[p])

    def e1_fwd(j, p):
        ch = own0 + j
        at = ex1.at[ch // PER, half(ch), :]
        return rcopy(at, at, e1fwd.at[j, p], e1recv.at[ch], peers[p])

    def h2_save(j):
        ch = own0 + j
        return lcopy(sv.at[1], hx2.at[ch // PER, half(ch), :], os_x.at[0])

    def e1_save(j, b):
        ch = own0 + j
        return lcopy(sv.at[b], ex1.at[ch // PER, half(ch), :], os_x.at[b])

    def h_out(j):
        return rcopy(own(tgt, j), own(hs, j), hsend.at[j], hrecv.at[own0 + j], nxt)

    def e_out(j):
        return rcopy(eout.at[half(j), :], own(es, j), esend.at[j], erecv.at[own0 + j], prv)

    def l_peer(p):
        return rcopy(lmine, lbuf.at[q], lsend.at[p], lrecv.at[q], peers[p])

    def l_out(kk):
        return rcopy(loss_out, loss_out, lout_s.at[kk], lout_r, (kk // PER, PER * q + kk % PER))

    def wait_chunk(buf, sems, ch):
        rcopy(own(buf, 0), own(buf, 0), hfwd.at[0, 0], sems.at[ch], peers[0]).wait_recv()

    def s_out_own(l, ch, b):
        return lcopy(sb.at[b, half(ch), :], s_hbm.at[l, ch // PER, half(ch), :], os_s.at[b])

    def g_out_own(l, ch, b):
        return lcopy(gb.at[b, half(ch), :], g_hbm.at[l, ch // PER, half(ch), :], os_g.at[b])

    def q_out_own(l, j, b):
        return lcopy(qb.at[b, HEAD, :], q_hbm.at[l, j // PER, half(j), :], os_q.at[b])

    def f_drain(b):
        s_out_own(0, 0, b).wait()
        g_out_own(0, 0, b).wait()

    def f_drain_all():
        for b in range(PER):
            f_drain(b)

    def f_outs(l, pr, b):
        return lcopy(sb.at[b], s_hbm.at[l, pr], os_s.at[b]), lcopy(gb.at[b], g_hbm.at[l, pr], os_g.at[b])

    def s_in_own(l, ch, b):
        return lcopy(s_hbm.at[l, ch // PER, half(ch), :], sb.at[b, HEAD, :], is_s.at[b])

    def b_ins(l, pr, b):
        return lcopy(s_hbm.at[l, pr], sb.at[b], is_s.at[b]), lcopy(g_hbm.at[l, pr], gb.at[b], is_g.at[b])

    def w_ins(l, jp, b):
        return lcopy(q_hbm.at[l, jp], qb.at[b], is_q.at[b]), lcopy(g_hbm.at[l, PER * q + jp], gb.at[b], is_g.at[b])

    def h_in(pr, b):
        return lcopy(hx.at[pr], hb.at[b], is_h.at[b])

    def e_in(pr, b):
        return lcopy(ex.at[pr], eb.at[b], is_e.at[b])

    def h2_in(pr, b):
        return lcopy(hx2.at[pr], tgt.at[b], is_x.at[b])

    def e1_in(pr, b):
        return lcopy(ex1.at[pr], tgt.at[b], is_x.at[b])

    def wait_pair(sems, pr):
        wait_chunk(hs, sems, PER * pr)
        wait_chunk(hs, sems, PER * pr + 1)

    def ob_save(b):
        return lcopy(eb.at[b], ex1.at[PER * q + 1], os_x.at[b])

    first, last = k == 0, k == 7
    mid = (k > 0) & (k < 7)
    high = k >= 4

    def flag(x):
        return jnp.where(x, 1, 0)

    m = 6 * flag(k < 3) + 4 * flag(k == 3) + 3 * flag(k == 4) + 2 * flag(k == 5)
    end = jnp.where(mid, 22, 18)

    def within(t, a, b):
        return (t >= a) & (t < b)

    def is_tr(t):
        return t == jnp.where(high, 0, 4)

    def is_bx(t):
        return last & ((t == 3) | (t == 6))

    def bx_jp(t):
        return t // 6

    def is_f_own(t):
        return within(t, 0, jnp.where(last, 3, 5)) & jnp.logical_not(is_tr(t))

    def is_f_two(t):
        return last & (t == 4)

    def f_own_j(t):
        return jnp.where(high, t - 1, t)

    def is_b_own(t):
        return mid & (within(t, 5 + m, 7 + m) | within(t, 8 + m, 10 + m))

    def b_own_j(t):
        return t - 5 - m - flag(t > 7 + m)

    def is_w(t):
        return mid & (within(t, jnp.where(high, 15, 10 + m), jnp.where(high, 17, 11 + m)) | (is_gap(t) & jnp.logical_not(high)))

    def w_jp(t):
        return jnp.where(high, t - 15, flag(t > 7 + m))

    def is_ob(t):
        return first & ((t == 11) | (t == 14))

    def ob_jp(t):
        return t // 14

    def is_gap(t):
        return mid & (t == 7 + m)

    def is_b_oth(t):
        return (mid & within(t, 17, 23)) | (first & within(t, 11, 19)) | (last & within(t, 13, 19))

    def is_f_oth(t):
        return (first & within(t, 5, 11)) | (last & within(t, 7, 13)) | (is_gap(t) & high) | (mid & (within(t, 5, 5 + m) | within(t, jnp.where(high, 10, 11) + m, jnp.where(high, 15, 17))))

    def oth_pair(i):
        return 2 * ((q + 1 + i % 3) % 4) + i // 3

    def f_pair(t):
        i = jnp.where(t < 5 + m, t - 5, jnp.where(is_gap(t), m, jnp.where(high, t - 9, t - 11)))
        return oth_pair(jnp.where(last, t - 7, i))

    def b_pair(t):
        i0 = jnp.where(t < 14, t - 12, t - 13)
        i = jnp.where(first, i0, jnp.where(last, t - 13, t - 17))
        return jnp.where(is_ob(t), PER * q + ob_jp(t), oth_pair(jnp.maximum(i, 0)))

    def is_loader(t):
        return is_b_own(t) | is_w(t) | is_b_oth(t)

    def start_load(t, li, b):
        l = TOP - li

        @pl.when(is_b_own(t))
        def _():
            s_in_own(l, own0 + b_own_j(t), b).start()

        @pl.when(is_w(t))
        def _():
            start_all(w_ins(l, w_jp(t), b))

        @pl.when(is_b_oth(t))
        def _():
            start_all(b_ins(l, b_pair(t), b))

    def next_load(t, li, b):
        @pl.when(li < 2)
        def _():
            start_load(t, li + 1, 1 - b)

        @pl.when(li == TOP)
        def _():
            start_load(t + 1, 0, 1 - b)

    def first_load(t):
        @pl.when(is_f_oth(t - 1))
        def _():
            wait_all(f_outs(2, 0, flip(t)))

        @pl.when(is_f_own(t - 1))
        def _():
            f_drain_all()

        @pl.when(jnp.logical_not(is_loader(t - 1) | is_f_oth(t - 1) | is_f_own(t - 1)))
        def _():
            start_load(t, 0, t % PER)

    def pre_h(t):
        @pl.when(is_f_oth(t + 1))
        def _():
            pr = f_pair(t + 1)
            wait_chunk(hs, hrecv, PER * pr)
            wait_chunk(hs, hrecv, PER * pr + 1)
            h_in(pr, flip(t)).start()

    def pre_e(t):
        @pl.when(is_b_oth(t + 1) & jnp.logical_not(is_ob(t + 1)))
        def _():
            pr = b_pair(t + 1)
            wait_chunk(es, erecv, PER * pr)
            wait_chunk(es, erecv, PER * pr + 1)
            e_in(pr, flip(t)).start()

    def wait_reload(t, l):
        @pl.when(t == jnp.where(last, 7, 5))
        def _():
            wait_all(w_reload(l))

    def tr_step(t):
        def zero(i, carry):
            r = pl.ds(pl.multiple_of(i * 8, 8), 8)
            for l in range(NL):
                acc1[l, r, :] = jnp.zeros((8, F), f32)
                acc2[l, r, :] = jnp.zeros((8, F), f32)
            return carry

        lax.fori_loop(0, DS // 8, zero, 0)

        @pl.when(jnp.logical_not(high))
        def _():
            f_drain_all()

        stage = [hb.at[0], hb.at[1], eb.at[0], eb.at[1], eout]
        pend_q, pend_h = [None] * 2, [None] * 5

        def reload(l):
            @pl.when(jnp.logical_not(high))
            def _():
                start_all(w_reload(l))

        def put(pend, sems, n, buf, src, dst):
            if pend[n] is not None:
                pend[n].wait()
            for o in range(0, src.shape[0], D):
                buf[:, o:o + D] = src[o:o + D, :].T
            pend[n] = lcopy(buf, dst, sems.at[n])
            pend[n].start()

        for l in range(NL):
            @pl.when(high)
            def _():
                wait_all(w_load(l))

            for i in range(3):
                put(pend_q, tr_q, i % PER, qb.at[i % PER], wb.at[l, :, pl.ds(i * 256, 256)], wta.at[l, pl.ds(i * 256, 256), :])
                for r in range(4 * i, 4 * i + 4):
                    put(pend_h, tr_h, r % 5, stage[r % 5], wa.at[l, :, pl.ds(r * 256, 256)], wtb.at[l, pl.ds(r * 256, 256), :])
            if l > 0:
                reload(l - 1)
        wait_all(pend_q + pend_h)
        reload(NL - 1)
        pre_h(t)

    def top_grads(jp, rows, h):
        diff = h.astype(f32) - tgt[jp, rows, :].astype(f32)
        es[jp, rows, :] = (diff * inv_total).astype(bf16)
        sq = jnp.sum((diff * diff).reshape(h.shape[0] // 8, 8, D), axis=0)
        ltile[...] += sum(sq[:, i:i + 128] for i in range(0, D, 128))

    def f_two(t):
        pr = PER * q + 1
        for j in range(2, 4):
            wait_chunk(hs, hrecv, own0 + j)
            for p in PEERS:
                h_fwd(j, p).start()
        hb[0] = hs[1]

        def layer(l, carry):
            b = l % PER

            @pl.when(l == TOP)
            def _():
                wait_all(f_outs(0, pr, 0))
                for i in range(PER):
                    sv[i] = hb[0, i * CH:(i + 1) * CH, :]

            h = hb[0]
            hT[l, pr] = nt(sel[...], h).astype(bf16)
            va[...] = h.astype(f32)

            def up(o):
                g, slope = gelu_and_slope(nn(h, wa[l, :, o:o + FB]))
                sb[b, :, o:o + FB] = slope
                g = g.astype(bf16)
                gb[b, :, o:o + FB] = g
                return g

            hb[0] = two_matmuls(va, up, lambda o, g: nn(g, wb[l, o:o + FB, :])).astype(bf16)
            start_all(f_outs(l, pr, b))
            return carry

        each_layer(layer)
        lcopy(y_in, tgt.at[1], trecv.at[1]).wait()
        for i in range(PER):
            rows = slice(i * CH, (i + 1) * CH)
            top_grads(1, rows, hb[0, rows, :])
        lmine[...] = ltile[...]
        saves = [lcopy(sv.at[i], hx2.at[pr, pl.ds(i * CH, CH), :], os_x.at[i]) for i in range(PER)]
        start_all(saves)
        wait_all(saves)
        for j in range(2, 4):
            for p in PEERS:
                h2_fwd(j, p).start()

    def f_own(t):
        j = f_own_j(t)
        ch = own0 + j
        rows = half(j)
        wait_chunk(hs, hrecv, ch)
        for p in PEERS:
            h_fwd(j, p).start()
        hc[...] = hs[j // PER, rows, :]

        def layer(l, carry):
            b = l % PER

            @pl.when((j == 0) & jnp.logical_not(high))
            def _():
                wait_all(w_load(l))

            @pl.when((l == TOP) | is_f_own(t - 1))
            def _():
                f_drain(b)

            @pl.when((k == 6) & (j == 3) & (l == 1))
            def _():
                for i in range(PER):
                    start_load(t + 1, i, 1 - i)

            h = hc[...]

            sv[jnp.maximum(l - 1, 0)] = h
            acc = va.at[HEAD, :]
            acc[...] = h.astype(f32)

            def up(o):
                g, slope = gelu_and_slope(nn(h, wa[l, :, o:o + FB]))
                sb[b, rows, o:o + FB] = slope
                g = g.astype(bf16)
                gb[b, rows, o:o + FB] = g
                return g

            hc[...] = two_matmuls(acc, up, lambda o, g: nn(g, wb[l, o:o + FB, :])).astype(bf16)
            s_out_own(l, ch, b).start()
            g_out_own(l, ch, b).start()

            @pl.when((j == 3) & within(k, 4, 6))
            def _():
                start_all(w_reload(l))

            @pl.when((j == 3) & (k == 6) & (l == TOP))
            def _():
                for i in reversed(range(NL)):
                    start_all(w_reload(i))

            return carry

        each_layer(layer)

        @pl.when(k < 7)
        def _():
            tgt[j // PER, rows, :] = hc[...]
            h_out(j).start()

        @pl.when(k == 7)
        def _():
            @pl.when(j == 0)
            def _():
                rcopy(y_in, tgt.at[0], tsend.at[0], trecv.at[0], partner).wait_recv()

            top_grads(j // PER, rows, hc[...])

        h2_save(j).start()
        hT[0, ch // PER, :, rows] = nt(sel[...], hs[j // PER, rows, :]).astype(bf16)
        for l in range(1, NL):
            hT[l, ch // PER, :, rows] = nt(sel[...], sv[l - 1]).astype(bf16)
        h2_save(j).wait()
        for p in PEERS:
            h2_fwd(j, p).start()
        pre_h(t)

    def q_drain(t, li):
        @pl.when((li == flag(is_b_own(t))) & is_b_own(t - 1))
        def _():
            q_out_own(0, 0, flip(t)).wait()

    def f_oth(t):
        pr = f_pair(t)
        hi = t % PER

        @pl.when(is_f_own(t - 1))
        def _():
            f_drain_all()

        q_drain(t, 0)

        @pl.when((k < 7) & (t == 5 + 2 * flag(k == 6)))
        def _():
            for j in range(4):
                h_out(j).wait_send()

        h_in(pr, hi).wait()

        def layer(l, carry):
            b = (t + l) % PER
            wait_reload(t, l)

            if not isinstance(l, int):
                @pl.when((l == 1) & is_f_oth(t - 1))
                def _():
                    wait_all(f_outs(2, 0, b))

                @pl.when(l == 1)
                def _():
                    wait_pair(h2recv, pr)
                    h2_in(pr, hi).start()
                    pre_h(t)
                    pre_e(t)

                @pl.when(l == TOP)
                def _():
                    wait_all(f_outs(0, pr, b))
                    h2_in(pr, hi).wait()
                    hb[hi] = tgt[hi]

            h = hb[hi]
            hT[l, pr] = nt(sel[...], h).astype(bf16)

            def up(o):
                g, slope = gelu_and_slope(nt(h, wb[l, o:o + FB, :]))
                sb[b, :, o:o + FB] = slope
                g = g.astype(bf16)
                gb[b, :, o:o + FB] = g
                return g

            if isinstance(l, int):
                va[...] = h.astype(f32)
                hb[hi] = two_matmuls(va, up, lambda o, g: nt(g, wa[l, :, o:o + FB])).astype(bf16)
            else:
                for o in BLOCKS:
                    up(o)
            start_all(f_outs(l, pr, b))
            return carry

        each_layer(layer, peel=True)
        wait_all(f_outs(1, pr, flip(t)))

        @pl.when(is_loader(t + 1))
        def _():
            start_load(t + 1, 0, flip(t))

    def b_own(t):
        j = b_own_j(t)
        ch = own0 + j
        jp = j // PER
        first_load(t)
        wait_chunk(es, erecv, ch)
        for p in PEERS:
            e_fwd(j, p).start()
        ec[...] = es[jp, half(j), :]

        def layer(li, carry):
            l = TOP - li
            b = (t + li) % PER
            s_in_own(l, ch, b).wait()
            q_drain(t, li)

            @pl.when(li == TOP)
            def _():
                q_out_own(2, j, b).wait()
                q_out_own(1, j, 1 - b).wait()


            @pl.when((li > 0) | jnp.logical_not(is_f_own(t - 1)))
            def _():
                next_load(t, li, b)

            wait_reload(t, l)
            e = ec[...]

            sv[jnp.maximum(li - 1, 0)] = e
            acc = va.at[HEAD, :]
            acc[...] = e.astype(f32)

            def up(o):
                p = nn(e, wa[l, :, o:o + FB]).astype(bf16).astype(f32)
                qv = (p * sb[b, HEAD, o:o + FB]).astype(bf16)
                qb[b, HEAD, o:o + FB] = qv
                return qv

            ec[...] = two_matmuls(acc, up, lambda o, qv: nn(qv, wb[l, o:o + FB, :])).astype(bf16)
            q_out_own(l, j, b).start()
            return carry

        each_layer(layer)
        @pl.when(j >= 2)
        def _():
            e_out(j - 2).wait_send()

        eout[half(j), :] = ec[...]
        e_out(j).start()
        e1_save(j, 1).start()
        eTs[jp, 2, :, half(j)] = nt(sel[...], es[jp, half(j), :]).astype(bf16)
        for li in range(1, NL):
            eTs[jp, TOP - li, :, half(j)] = nt(sel[...], sv[li - 1]).astype(bf16)
        e1_save(j, 1).wait()

        @pl.when(j == jnp.where(k > 1, 1, 2))
        def _():
            for i in range(2):
                for p in PEERS:
                    e1_fwd(i, p).start()

        @pl.when(j == 3)
        def _():
            for i in range(2, 4):
                for p in PEERS:
                    e1_fwd(i, p).start()

        pre_e(t)
        pre_h(t)

    def wgrad(l, hTl, eTl, b):
        for o in range(0, F, FW):
            acc1[l, :, o:o + FW] += nn(hTl, qb[b, :, o:o + FW])
            acc2[l, :, o:o + FW] += nn(eTl, gb[b, :, o:o + FW])

    def bx_step(t):
        jp = bx_jp(t)
        pr = PER * q + jp
        eb[0] = es[jp]

        def layer(li, carry):
            l = TOP - li
            b = li % PER

            @pl.when(li == 1)
            def _():
                @pl.when(jp == 0)
                def _():
                    f_drain_all()

                @pl.when(jp == 1)
                def _():
                    for bb in range(PER):
                        wait_all(f_outs(0, pr, bb))

                start_all(b_ins(0, pr, 0))

            @pl.when(li == TOP)
            def _():
                wait_all(b_ins(0, pr, 0))
                for i in range(2):
                    sv[i] = eb[0, i * CH:(i + 1) * CH, :]

            e = eb[0]
            eT = nt(sel[...], e).astype(bf16)
            va[...] = e.astype(f32)

            def up(o):
                p = nt(e, wb[l, o:o + FB, :]).astype(bf16).astype(f32)
                qv = (p * sb[b, :, o:o + FB]).astype(bf16)
                qb[b, :, o:o + FB] = qv
                return qv

            eb[0] = two_matmuls(va, up, lambda o, qv: nt(qv, wa[l, :, o:o + FB])).astype(bf16)

            @pl.when(li == TOP)
            def _():
                @pl.when(jp == 1)
                def _():
                    for i in range(2):
                        e_out(i).wait_send()

                eout[...] = eb[0]
                for i in range(2):
                    e_out(PER * jp + i).start()
                for i in range(2):
                    e1_save(PER * jp + i, i).start()

            wgrad(l, hT[l, pr], eT, b)

            @pl.when(jp == 1)
            def _():
                start_all(w_reload(l))

            return carry

        each_layer(layer)
        for i in range(2):
            e1_save(PER * jp + i, i).wait()

        @pl.when(jp == 1)
        def _():
            for p in PEERS:
                l_peer(p).start()
            for pair in (0, 2):
                for fwd in (e_fwd, e1_fwd):
                    for i in (pair, pair + 1):
                        for p in PEERS:
                            fwd(i, p).start()
            pre_h(t)

    def w_step(t):
        jp = w_jp(t)
        q_drain(t, 0)

        @pl.when(is_f_oth(t - 1))
        def _():
            wait_all(f_outs(2, 0, flip(t)))

        start_load(t, 1, flip(t))

        def layer(li, carry):
            l = TOP - li
            b = (t + li) % PER
            wait_all(w_ins(l, jp, b))

            @pl.when(li == 1)
            def _():
                pre_h(t)
                pre_e(t)

            wgrad(l, hT[l, PER * q + jp], eTs[jp, l], b)

            @pl.when(li == 0)
            def _():
                start_load(t, 2, b)

            @pl.when(li == 1)
            def _():
                start_load(t + 1, 0, b)

            return carry

        each_layer(layer)

    half_own = pl.ds(pl.multiple_of(96 * c, 8), 96)
    half_oth = pl.ds(pl.multiple_of(96 * (1 - c), 8), 96)

    def final_copies(l):
        lg = NL * c + l
        return [
            rcopy(acc1.at[l, half_oth, :], out_up.at[lg], xo_s.at[l, 0], xo_r.at[l, 0], partner),
            rcopy(acc2.at[l, half_oth, :], out_down.at[lg], xo_s.at[l, 1], xo_r.at[l, 1], partner),
            lcopy(acc1.at[l, half_own, :], out_up.at[lg], lo_s.at[l, 0]),
            lcopy(acc2.at[l, half_own, :], out_down.at[lg], lo_s.at[l, 1]),
        ]

    def b_oth(t):
        pr = b_pair(t)
        ei = t % PER
        inner = jnp.logical_not(first) | (t > 16)
        first_load(t)

        for j, at in ((0, 11), (1, 11), (2, 13), (3, 14)):
            @pl.when(first & (t == at))
            def _():
                wait_chunk(es, erecv, own0 + j)
                for p in PEERS:
                    e_fwd(j, p).start()

        @pl.when(is_ob(t))
        def _():
            eb[ei] = es[ob_jp(t)]

        @pl.when(jnp.logical_not(is_ob(t)))
        def _():
            e_in(pr, ei).wait()

        def layer(li, carry):
            l = TOP - li
            b = (t + li) % PER
            wait_all(b_ins(l, pr, b))
            q_drain(t, li)
            next_load(t, li, b)

            if not isinstance(li, int):
                @pl.when(li == jnp.where(is_ob(t), 2, 1))
                def _():
                    pre_e(t)

                @pl.when((li == 1) & inner)
                def _():
                    wait_pair(e1recv, pr)
                    e1_in(pr, ei).start()

                @pl.when((li == TOP) & inner)
                def _():
                    e1_in(pr, ei).wait()
                    eb[ei] = tgt[ei]

                @pl.when((li == TOP) & first & (t == 14))
                def _():
                    ob_save(ei).start()

            e = eb[ei]
            eT = nt(sel[...], e).astype(bf16)
            for o in range(0, F, FW):
                p = nn(e, wa[l, :, o:o + FW]).astype(bf16).astype(f32)
                qb[b, :, o:o + FW] = (p * sb[b, :, o:o + FW]).astype(bf16)
            if isinstance(li, int):
                for o in range(0, D, DW):
                    eb[ei, :, o:o + DW] = (e[:, o:o + DW].astype(f32) + nn(qb[b], wb[l, :, o:o + DW])).astype(bf16)
            wgrad(l, hT[l, pr], eT, b)

            if not isinstance(li, int):
                @pl.when((li == 1) & jnp.logical_not(inner))
                def _():
                    for o in range(0, D, DW):
                        eb[ei, :, o:o + DW] = (eb[ei, :, o:o + DW].astype(f32) + nn(qb[b], wb[l, :, o:o + DW])).astype(bf16)

            @pl.when(t == end)
            def _():
                start_all(final_copies(l))

            return carry

        each_layer(layer, peel=True)

        @pl.when(first & (t == 14))
        def _():
            ob_save(ei).wait()
            for j in range(2, 4):
                for p in PEERS:
                    e1_fwd(j, p).start()

        @pl.when(last & (t == 13))
        def _():
            for p in PEERS:
                qo = (q + 1 + p) % 4
                rcopy(lmine, lbuf.at[qo], lsend.at[p], lrecv.at[qo], peers[p]).wait_recv()
            lbuf[q] = lmine[...]
            tot = (lbuf[0] + lbuf[1]) + (lbuf[2] + lbuf[3])
            loss_out[...] = jnp.zeros((8, 128), f32) + jnp.sum(tot) * (0.5 * inv_total)
            for kk in range(7):
                l_out(kk).start()

    def step(t, carry):
        for test, run in ((is_tr, tr_step), (is_f_own, f_own), (is_f_oth, f_oth), (is_b_own, b_own), (is_bx, bx_step), (is_f_two, f_two), (is_w, w_step), (is_b_oth, b_oth)):
            @pl.when(test(t))
            def _():
                run(t)

        return carry

    lax.fori_loop(0, NSTEP, step, 0)

    @pl.when(first)
    def _():
        wait_pair(e1recv, oth_pair(3))

    for j in range(4):
        for p in PEERS:
            h_fwd(j, p).wait_send()
            e_fwd(j, p).wait_send()
            h2_fwd(j, p).wait_send()

    for j in range(4):
        @pl.when((k > 0) | (j > 1))
        def _():
            for p in PEERS:
                e1_fwd(j, p).wait_send()

    @pl.when(k > 0)
    def _():
        for j in range(2, 4):
            e_out(j).wait_send()

    @pl.when(k < 7)
    def _():
        l_out(0).wait_recv()

    @pl.when(k == 1)
    def _():
        xcopy(0).wait_send()
        xcopy(1).wait_send()

    @pl.when(k == 6)
    def _():
        tcopy().wait_send()

    @pl.when(k == 7)
    def _():
        for p in PEERS:
            l_peer(p).wait_send()
        for kk in range(7):
            l_out(kk).wait_send()

    for l in range(NL):
        lg = NL * (1 - c) + l
        rcopy(acc1.at[l, half_oth, :], out_up.at[lg], xo_s.at[l, 0], xo_r.at[l, 0], partner).wait_recv()
        rcopy(acc2.at[l, half_oth, :], out_down.at[lg], xo_s.at[l, 1], xo_r.at[l, 1], partner).wait_recv()
        r1, r2, l1, l2 = final_copies(l)
        r1.wait_send()
        r2.wait_send()
        l1.wait()
        l2.wait()


def solution(mesh):
    n_data = mesh.shape["data"]

    def per_device(inputs, targets, w_up, w_down):
        n_micro, n_tok, width = inputs.shape
        inv_total = 1.0 / (n_data * n_micro * n_tok)
        x = inputs.reshape(n_micro * n_tok, width)
        y = targets.reshape(n_micro * n_tok, width)
        V = pltpu.VMEM
        DMA = pltpu.SemaphoreType.DMA
        S = jax.ShapeDtypeStruct
        anyspec = pl.BlockSpec(memory_space=pl.ANY)
        pairs = 8
        half_grad = S((PER * NL, D // pairs, F), f32)
        rows = S((pairs, PR, D), bf16)
        two_rows = V((PER, PR, D), bf16)
        two_wide = V((PER, PR, F), bf16)
        grads = V((NL, DS, F), f32)
        tile = V((8, 128), f32)
        two, four, by_layer, chunks, fan = DMA((PER,)), DMA((4,)), DMA((NL, PER)), DMA((16,)), DMA((4, 3))
        outs = pl.pallas_call(
            functools.partial(kernel, inv_total),
            out_shape=(
                S((8, 128), f32), half_grad, half_grad,
                S((NL, pairs, PR, F), f32), S((NL, pairs, PR, F), bf16), S((NL, PER, PR, F), bf16),
                S((NL, D, F), bf16), S((NL, F, D), bf16), rows, rows, rows, rows,
            ),
            in_specs=[anyspec] * 4,
            out_specs=(pl.BlockSpec(memory_space=pltpu.VMEM),) + (anyspec,) * 11,
            scratch_shapes=[
                V((NL, D, F), bf16), V((NL, F, D), bf16), grads, grads, two_rows, two_rows,
                V((PER, PR, F), f32), two_wide, two_wide,
                V((NL, pairs, DS, PR), bf16), V((PER, NL, DS, PR), bf16),
                two_rows, two_rows, V((PR, D), bf16), two_rows, V((PER, CH, D), bf16), V((PR, D), f32),
                V((DS, D), bf16), tile, V((4, 8, 128), f32), tile,
                by_layer, by_layer, chunks, chunks, fan, fan, two, two, chunks, chunks, two, four, two,
                fan, fan, four, four, DMA((1,)), DMA((3,)), DMA((7,)), DMA,
            ] + [two] * 9 + [DMA((6,)), by_layer, by_layer, by_layer],
            compiler_params=pltpu.CompilerParams(collective_id=0, has_side_effects=True, vmem_limit_bytes=67043328),
            name="stack_step",
        )(x, y, w_up, w_down)
        return outs[0][0, 0], outs[1], jnp.swapaxes(outs[2], 1, 2)

    return jax.shard_map(
        per_device,
        mesh=mesh,
        in_specs=(P("data", None, None), P("data", None, None), P("stage", None, None), P("stage", None, None)),
        out_specs=(P(), P("stage", "data", None), P("stage", None, "data")),
        check_vma=False,
    )
```
